32 devices in a mesh: rows: 4 (over z), cols: 8 (over y, x, core).
Axes of the slice: x: 2, y: 2, z: 4, core: 2. Of those that a mesh axis runs over, the one named last changes fastest.
Arguments:
- features: bfloat16 [65536, 440], P(('rows', 'cols')), may hold values from -12 to 12
- residual: float32 [65536, 147], P(('rows', 'cols')), may hold values from -6 to 6
- coeffs: float32 [65536, 147], P(('rows', 'cols')), may hold values from -3 to 3
- block_inverse: float32 [2, 2048, 2048], P(None, ('rows', 'cols')), may hold values from -0.0234375 to 0.0234375
- block_index: int32 [2, 2048], P(None, 'cols'), may hold values from 0 to 2047, as said below
- owners: int32 [2], replicated, may hold values from 0 to 3
Outputs:
- new_coeffs: float32 [65536, 147], P(('rows', 'cols'))
- new_residual: float32 [65536, 147], P(('rows', 'cols'))
The draws below stay inside these ranges and needn't reach their ends.
Inputs may be any that keep to these rules, and one draw needn't show every extreme that they name: `block_index`: for each step and each aligned run of 256 positions, the indices are distinct.
All inputs are finite; a program needn't handle non-finite values.
Results may differ from the reference program's by a relative error of at most 0.0028.
Values may be sent and summed in bfloat16 or wider, within the bound.
No kernel may reach another device: no remote copies, remote signals or barrier semaphores. Data moves between devices by JAX's collectives and lax.ppermute only.
A program may use at most 64 MiB of HBM per device.

```python
import jax
import jax.numpy as jnp
from jax import lax

D = 440
C = 147
BLOCK = 2048
STEPS = 2
FRAMES_DEV = 2048
FRAMES = 65536
PICK = 256
N_ROWS = 4
N_COLS = 8


def draw_block_index(key, part):
    per_col = BLOCK // N_COLS
    streams = jax.random.split(jax.random.fold_in(key, 17), STEPS * N_COLS)
    picked = jax.vmap(lambda stream: jax.random.permutation(stream, FRAMES_DEV)[:per_col])(streams)
    return picked.reshape(STEPS, BLOCK).astype(jnp.int32)


def draw_features(key, part):
    latent_width = 32
    cluster_count = 64
    streams = [jax.random.fold_in(key, 211 + offset) for offset in range(8)]
    mixing = jax.random.normal(streams[0], (latent_width, D), jnp.float32) / jnp.sqrt(float(latent_width))
    centres = jax.random.normal(streams[1], (cluster_count, latent_width), jnp.float32)
    member = jax.random.randint(streams[2], (FRAMES,), 0, cluster_count)
    spread = jnp.full((cluster_count, 1), 0.3, jnp.float32)
    local_part = jax.random.normal(streams[5], (FRAMES, latent_width), jnp.float32)
    jitter_scale = jnp.exp(jax.random.uniform(streams[7], (FRAMES, 1), jnp.float32, jnp.log(0.4), jnp.log(1.0)))
    frame_latent = centres[member] + local_part * spread[member]
    jitter = jitter_scale * jax.random.normal(streams[6], (FRAMES, D), jnp.float32)
    mixed = jnp.dot(frame_latent, mixing, precision=jax.lax.Precision.HIGHEST) + jitter
    return jnp.clip(mixed, -12.0, 12.0).astype(jnp.bfloat16)


def shard_levels(key, dims, cuts, smallest, top_value):
    def one(position, blocks):
        draws = jax.random.uniform(jax.random.fold_in(jax.random.fold_in(key, 6), position), (blocks,), jnp.float32, smallest / len(cuts), top_value / len(cuts))
        return jnp.repeat(jnp.exp(draws), dims[position] // blocks).reshape((-1,) + (1,) * (len(dims) - position - 1))

    factor_of = one(*cuts[0])
    for cut in cuts[1:]:
        factor_of = factor_of * one(*cut)
    return factor_of


def noise(key, dims, deviation, bound, cuts=(), held_as=jnp.bfloat16):
    values = deviation * jax.random.normal(key, dims, jnp.float32)
    if cuts:
        values = values * shard_levels(key, dims, cuts, -0.22, 0.18)
    return jnp.clip(values, -bound, bound).astype(held_as)


def setup_inputs(seed: int = 0) -> dict:
    arg_keys = jax.random.split(jax.random.key(seed), 7)
    return {
        "features": draw_features(jax.random.fold_in(arg_keys[6], 71), 0),
        "residual": noise(arg_keys[1], (FRAMES, C), 1.0, 6.0, ((0, 32),), jnp.float32),
        "coeffs": noise(arg_keys[2], (FRAMES, C), 0.5, 3.0, ((0, 32),), jnp.float32),
        "block_inverse": noise(arg_keys[3], (STEPS, BLOCK, BLOCK), (36 * BLOCK) ** -0.5, 0.0234375, ((1, 32),), jnp.float32),
        "block_index": draw_block_index(jax.random.fold_in(arg_keys[6], 71), 0),
        "owners": jax.random.randint(arg_keys[5], (STEPS,), 0, N_ROWS).astype(jnp.int32),
    }


def reference(features, residual, coeffs, block_inverse, block_index, owners):
    total = features.shape[0]
    squares = jnp.sum(jnp.square(features.astype(jnp.float32)), axis=1)
    row_block = min(4096, total)
    feature_blocks = features.reshape(total // row_block, row_block, D)
    norm_blocks = squares.reshape(total // row_block, row_block)
    column_group = (jnp.arange(BLOCK) // PICK).astype(jnp.int32)
    for step_id in range(STEPS):
        points = ((owners[step_id] * N_COLS + column_group) * FRAMES_DEV + block_index[step_id]).astype(jnp.int32)
        chosen = features[points]
        chosen_norms = squares[points]
        update = jnp.dot(block_inverse[step_id], residual[points], precision=lax.Precision.HIGHEST,
                         preferred_element_type=jnp.float32).astype(jnp.bfloat16)

        def kernel_rows(operands):
            block_rows, block_norms = operands
            inner = jnp.dot(block_rows, chosen.T, preferred_element_type=jnp.float32)
            distance = block_norms[:, None] + chosen_norms[None, :] - 2.0 * inner
            kernel = jnp.exp(distance * (-1.0 / D)).astype(jnp.bfloat16)
            return jnp.dot(kernel, update, preferred_element_type=jnp.float32)

        change = lax.map(kernel_rows, (feature_blocks, norm_blocks)).reshape(total, C)
        residual = residual - change
        residual = residual.at[points].add(-0.5 * update.astype(jnp.float32))
        coeffs = coeffs.at[points].add(update.astype(jnp.float32))
    return coeffs, residual
```

```python
import functools

import jax
import jax.numpy as jnp
from jax import lax
from jax.experimental import pallas as pl
from jax.experimental.pallas import tpu as pltpu
from jax.sharding import PartitionSpec as P


penalty = 0.5
LANES = 128
VMEM = pltpu.MemorySpace.VMEM
SMEM = pltpu.MemorySpace.SMEM
f32 = jnp.float32
bf16 = jnp.bfloat16
f16 = jnp.float16
MM = dict(preferred_element_type=f32)


def up(value, unit):
    return -(-value // unit) * unit


def params(megabytes=56):
    return pltpu.CompilerParams(vmem_limit_bytes=megabytes * 1024 * 1024)


def split(value, parts):
    pieces = []
    for _ in range(parts - 1):
        high = value.astype(bf16)
        pieces.append(high)
        value = value - high.astype(f32)
    pieces.append(value.astype(bf16))
    return pieces


def matmul(a, b):
    return lax.dot_general(a, b, (((1,), (0,)), ((), ())), **MM)


def matmul_nt(a, b):
    return lax.dot_general(a, b, (((1,), (1,)), ((), ())), **MM)


def one_hot(frames, index_row):
    rows = lax.broadcasted_iota(jnp.int32, (frames, index_row.shape[1]), 0)
    return jnp.where(rows == index_row, 1.0, 0.0).astype(bf16)


def pick_residual(index, residual_t):
    outputs, frames = residual_t.shape
    rows = up(outputs, 16)
    picks = index.shape[1]

    def body(index_ref, residual_ref, first_ref, second_ref):
        value = residual_ref[...]
        high, low = split(value, 2)
        both = jnp.concatenate(
            [jnp.pad(high, ((0, rows - outputs), (0, 0))), jnp.pad(low, ((0, rows - outputs), (0, 0)))], 0
        )
        first = matmul(both, one_hot(frames, index_ref[0:1, :]))
        first_ref[...] = first[:rows] + first[rows:]
        second = matmul(both, one_hot(frames, index_ref[1:2, :]))
        second_ref[...] = second.astype(bf16)

    return pl.pallas_call(
        body,
        out_shape=(
            jax.ShapeDtypeStruct((rows, picks), f32),
            jax.ShapeDtypeStruct((2 * rows, picks), bf16),
        ),
        compiler_params=params(),
        name="pick_residual",
    )(index, residual_t)


def norm_rows(squares, kinds):
    width = squares.shape[1]
    norm = split(-0.5 * squares, 3)
    ones = jnp.ones((3, width), bf16)
    zeros = jnp.zeros((6, width), bf16)
    norm = jnp.concatenate(norm, 0)
    pieces = []
    for kind in kinds:
        if kind == 0:
            pieces.append(zeros)
        elif kind == 1:
            pieces.append(jnp.concatenate([norm, ones], 0))
        else:
            pieces.append(jnp.concatenate([ones, norm], 0))
    return jnp.concatenate(pieces, 0)


def pick_features(index, index_t, same_owner, features_t, second_residual):
    width, frames = features_t.shape
    depth = up(width + 20, 16)
    picks = index.shape[1]
    extra = second_residual.shape[0]
    tail = depth - width

    def body(same_ref, index_ref, index_t_ref, features_ref, residual_ref, local_ref, first_ref, second_ref):
        features = features_ref[...]
        wide = features.astype(f32)
        squares = jnp.sum(wide * wide, axis=0, keepdims=True)
        local_ref[0:width, :] = features
        rest = jnp.zeros((tail - 18, frames), bf16)
        local_ref[width:depth, :] = jnp.concatenate([norm_rows(squares, (1, 1, 0)), rest], 0)

        hot = one_hot(frames, index_ref[0:1, :])
        picked = matmul(features, hot)
        picked_squares = jnp.sum(picked * picked, axis=0, keepdims=True)
        first_ref[0:width, :] = picked.astype(bf16)
        rest = jnp.zeros((tail - 18, picks), bf16)
        first_ref[width:depth, :] = jnp.concatenate([norm_rows(picked_squares, (2, 0, 1)), rest], 0)

        hot = one_hot(frames, index_ref[1:2, :])
        picked = matmul(features, hot)
        picked_squares = jnp.sum(picked * picked, axis=0, keepdims=True)
        second_ref[0:width, :] = picked.astype(bf16)
        places = lax.broadcasted_iota(jnp.int32, (picks, picks), 0) + 1
        meet = jnp.where(index_t_ref[:, 0:1] == index_ref[1:2, :], places, 0)
        place = jnp.max(meet, axis=0, keepdims=True) * same_ref[0]
        place = jnp.concatenate([place // LANES, place % LANES], 0).astype(f32).astype(bf16)
        rest = jnp.zeros((tail - 20, picks), bf16)
        second_ref[width:depth, :] = jnp.concatenate([norm_rows(picked_squares, (0, 2, 2)), place, rest], 0)
        second_ref[depth:, :] = residual_ref[...]

    vmem = pl.BlockSpec(memory_space=VMEM)
    return pl.pallas_call(
        body,
        in_specs=[pl.BlockSpec(memory_space=SMEM), vmem, vmem, vmem, vmem],
        out_shape=(
            jax.ShapeDtypeStruct((depth, frames), bf16),
            jax.ShapeDtypeStruct((depth, picks), bf16),
            jax.ShapeDtypeStruct((depth + extra, picks), bf16),
        ),
        compiler_params=params(),
        name="pick_features",
    )(same_owner, index, index_t, features_t, second_residual)


def lane_start(value, unit):
    return pl.ds(pl.multiple_of(value * unit, unit), unit)


def fold(update):
    half = update.shape[0] // 2
    return jnp.concatenate([update[:half], update[half:]], 1).astype(bf16)


def first_update(order, pieces, inverse, step):
    rows, picks = pieces[0].shape
    block = picks * len(pieces)
    mine = inverse.shape[1]

    def body(order_ref, inverse_ref, *refs):
        pieces_ref, out_ref, canon = refs[: len(pieces)], refs[-2], refs[-1]
        for k, piece in enumerate(pieces_ref):
            high, low = split(piece[...].astype(f32), 2)
            canon[0:rows, lane_start(order_ref[k], picks)] = high
            canon[rows:, lane_start(order_ref[k], picks)] = low
        high, low = split(inverse_ref[0], 2)
        product = matmul_nt(canon[...], jnp.concatenate([high, low], 0))
        product = product[:rows] + product[rows:]
        out_ref[...] = fold(product[:, :mine] + product[:, mine:])

    vmem = pl.BlockSpec(memory_space=VMEM)
    return pl.pallas_call(
        body,
        grid=(1,),
        in_specs=[pl.BlockSpec(memory_space=SMEM), pl.BlockSpec((1, mine, block), lambda i: (step, 0, 0))]
        + [vmem] * len(pieces),
        out_specs=vmem,
        out_shape=jax.ShapeDtypeStruct((rows // 2, 2 * mine), bf16),
        scratch_shapes=[pltpu.VMEM((2 * rows, block), bf16)],
        compiler_params=params(),
        name="first_update",
    )(order, inverse, *pieces)


def second_operator(order, first, second, inverse, step, width, scale):
    depth, picks = first[0].shape
    count = len(first)
    block = picks * count
    mine = inverse.shape[1]
    rows = (second[0].shape[0] - depth) // 2

    def body(order_ref, inverse_ref, *refs):
        first_ref, second_ref = refs[:count], refs[count : 2 * count]
        operator_ref, base_ref, canon, stacked, total = refs[2 * count :]
        for k in range(count):
            canon[:, lane_start(order_ref[k], picks)] = first_ref[k][...]
        high, low = split(inverse_ref[0], 2)
        stacked[0:mine, :] = high
        stacked[mine:, :] = low
        base = jnp.zeros((2 * rows, 2 * mine), f32)
        lanes = lax.broadcasted_iota(jnp.int32, (picks, picks), 1) + 1
        for k in range(count):
            here = order_ref[k]
            there = second_ref[k][0:depth, :]
            part = stacked[:, lane_start(here, picks)]
            base = base + matmul_nt(second_ref[k][depth:, :], part)
            turned = jnp.transpose(there)
            inner = matmul(turned, canon[...])
            kernel = jnp.exp2(inner * scale).astype(bf16)
            place = turned[:, width + 18 : width + 20].astype(f32)
            place = (place[:, 0:1] * LANES + place[:, 1:2]).astype(jnp.int32)
            meet = jnp.where(place == lanes, penalty, 0.0).astype(bf16)
            product = matmul(part, kernel)
            if k == 0:
                total[...] = product
            else:
                total[...] += product
            total[:, lane_start(here, picks)] += matmul(part, meet)
        operator = total[0:mine, :] + total[mine:, :]
        high, low = split(operator, 2)
        operator_ref[0:mine, :] = high
        operator_ref[mine:, :] = low
        base = base[:rows] + base[rows:]
        base_ref[...] = base[:, :mine] + base[:, mine:]

    vmem = pl.BlockSpec(memory_space=VMEM)
    flops = 2 * block * block * (depth + 2 * mine)
    return pl.pallas_call(
        body,
        grid=(1,),
        in_specs=[pl.BlockSpec(memory_space=SMEM), pl.BlockSpec((1, mine, block), lambda i: (step, 0, 0))]
        + [vmem] * (2 * count),
        out_specs=(vmem, vmem),
        out_shape=(
            jax.ShapeDtypeStruct((2 * mine, block), bf16),
            jax.ShapeDtypeStruct((rows, mine), f32),
        ),
        scratch_shapes=[
            pltpu.VMEM((depth, block), bf16),
            pltpu.VMEM((2 * mine, block), bf16),
            pltpu.VMEM((2 * mine, block), f32),
        ],
        cost_estimate=pl.CostEstimate(flops=flops, transcendentals=block * block, bytes_accessed=10**7),
        compiler_params=params(),
        name="second_operator",
    )(order, inverse, *first, *second)


def block_kernel(order, pieces, local, scale, name):
    depth, frames = local.shape
    picks = pieces[0].shape[1]
    count = len(pieces)
    block = picks * count

    def body(order_ref, local_ref, *refs):
        pieces_ref, out_ref = refs[:count], refs[-1]
        here = pl.program_id(0)
        for k in range(count):

            @pl.when(order_ref[k] == here)
            def _():
                turned = jnp.transpose(pieces_ref[k][0:depth, :])
                inner = matmul(turned, local_ref[...])
                out_ref[...] = jnp.exp2(inner * scale).astype(bf16)

    vmem = pl.BlockSpec(memory_space=VMEM)
    return pl.pallas_call(
        body,
        grid=(count,),
        in_specs=[pl.BlockSpec(memory_space=SMEM), vmem] + [vmem] * count,
        out_specs=pl.BlockSpec((picks, frames), lambda i: (i, 0)),
        out_shape=jax.ShapeDtypeStruct((block, frames), bf16),
        cost_estimate=pl.CostEstimate(
            flops=2 * block * frames * depth, transcendentals=block * frames, bytes_accessed=10**7
        ),
        compiler_params=params(),
        name=name,
    )(order, local, *pieces)


def unfold(order_ref, pieces_ref, parts, canon):
    half, width = pieces_ref[0].shape[0] // parts, pieces_ref[0].shape[1]
    mine = width // 2
    count = len(pieces_ref)
    lanes = lax.broadcasted_iota(jnp.int32, (half, width), 1)
    low = lanes < mine
    core = order_ref[parts * count // 2]
    for k in range(0, count, 2):
        for r in range(parts):
            here = pieces_ref[k][r * half : (r + 1) * half, :].astype(f32)
            other = pieces_ref[k + 1][r * half : (r + 1) * half, :].astype(f32)
            a = jnp.where(core == 0, here, other)
            b = jnp.where(core == 0, other, here)
            upper = jnp.where(low, a, pltpu.roll(b, mine, 1))
            lower = jnp.where(low, pltpu.roll(a, mine, 1), b)
            place = lane_start(order_ref[parts * (k // 2) + r], width)
            canon[0:half, place] = upper.astype(bf16)
            canon[half:, place] = lower.astype(bf16)


def second_update(order, pieces, operator, base):
    rows, mine = base.shape
    block = operator.shape[1]
    count = len(pieces)

    def body(order_ref, operator_ref, base_ref, *refs):
        pieces_ref, out_ref, canon = refs[:count], refs[-2], refs[-1]
        unfold(order_ref, pieces_ref, pieces[0].shape[0] * 2 // rows, canon)
        product = matmul_nt(canon[...], operator_ref[...])
        out_ref[...] = fold(base_ref[...] - (product[:, :mine] + product[:, mine:]))

    vmem = pl.BlockSpec(memory_space=VMEM)
    return pl.pallas_call(
        body,
        in_specs=[pl.BlockSpec(memory_space=SMEM)] + [vmem] * (2 + count),
        out_specs=vmem,
        out_shape=jax.ShapeDtypeStruct((rows // 2, 2 * mine), bf16),
        scratch_shapes=[pltpu.VMEM((rows, block), bf16)],
        compiler_params=params(),
        name="second_update",
    )(order, operator, base, *pieces)


def apply_update(scalars, order, pieces, kernel, index, step, residual_t, coeffs_t, name):
    outputs, frames = residual_t.shape
    block = kernel.shape[0]
    picks = index.shape[1]
    count = len(pieces)
    rows = up(outputs, 16)
    tile = min(512, frames)

    def body(scalars_ref, order_ref, index_ref, kernel_ref, residual_ref, coeffs_ref, *refs):
        pieces_ref = refs[:count]
        new_residual_ref, new_coeffs_ref, canon, own = refs[count:]
        here = pl.program_id(0)

        @pl.when(here == 0)
        def _():
            unfold(order_ref, pieces_ref, pieces[0].shape[0] * 2 // rows, canon)
            mine = canon[:, lane_start(scalars_ref[0], picks)].astype(f32)
            own[...] = (mine * scalars_ref[1 + step].astype(f32)).astype(bf16)

        change = matmul(canon[...], kernel_ref[...])
        frame = lax.broadcasted_iota(jnp.int32, (tile, picks), 0) + here * tile
        hot = jnp.where(frame == index_ref[step : step + 1, :], 1.0, 0.0).astype(bf16)
        put = matmul_nt(own[...], hot)
        new_residual_ref[...] = residual_ref[...] - (change + penalty * put)[:outputs]
        new_coeffs_ref[...] = coeffs_ref[...] + put[:outputs]

    vmem = pl.BlockSpec(memory_space=VMEM)
    smem = pl.BlockSpec(memory_space=SMEM)
    strip = pl.BlockSpec((outputs, tile), lambda i: (0, i))
    return pl.pallas_call(
        body,
        grid=(frames // tile,),
        in_specs=[smem, smem, vmem, pl.BlockSpec((block, tile), lambda i: (0, i)), strip, strip]
        + [vmem] * count,
        out_specs=(strip, strip),
        out_shape=(
            jax.ShapeDtypeStruct((outputs, frames), f32),
            jax.ShapeDtypeStruct((outputs, frames), f32),
        ),
        scratch_shapes=[pltpu.VMEM((rows, block), bf16), pltpu.VMEM((rows, picks), bf16)],
        cost_estimate=pl.CostEstimate(
            flops=2 * rows * block * frames, transcendentals=0, bytes_accessed=2 * block * frames
        ),
        compiler_params=params(),
        name=name,
    )(scalars, order, index, kernel, residual_t, coeffs_t, *pieces)


def meet_at(value, offset, rows, cols, row_step, chip_step, core_step):
    def partner(position):
        row, col = position // cols, position % cols
        chip, core = col // 2, col % 2
        return (row ^ row_step) * cols + (chip ^ chip_step) * 2 + (core ^ core_step)

    return lax.ppermute(value, ("rows", "cols"), [(i, partner(i)) for i in range(rows * cols)])


def per_device_pieces(rows, cols, features, residual, coeffs, block_inverse, block_index, owners):
    chips = cols // 2
    scale = 2.0 / features.shape[1] * 1.4426950408889634
    my_row = lax.axis_index("rows")
    my_col = lax.axis_index("cols")
    features_t, residual_t, coeffs_t = features.T, residual.T, coeffs.T
    send = functools.partial(meet_at, rows=rows, cols=cols, offset=0)

    def from_owner(value, owner):
        arrived = [value] + [send(value, row_step=k, chip_step=0, core_step=0) for k in range(1, rows)]
        chosen = arrived[0]
        for k in range(1, rows):
            chosen = jnp.where((my_row ^ k) == owner, arrived[k], chosen)
        return chosen

    def over_chips(values):
        return [v if k == 0 else send(v, row_step=0, chip_step=k, core_step=0) for v in values for k in range(chips)]

    def over_cores(values):
        return [w for v in values for w in (v, send(v, row_step=0, chip_step=0, core_step=1))]

    def over_rows(value):
        return [value] + [send(value, row_step=k, chip_step=0, core_step=0) for k in range(1, rows)]

    my_chip, my_core = my_col // 2, my_col % 2
    col_order = jnp.stack(
        [(my_chip ^ k) * 2 + (my_core ^ core) for k in range(chips) for core in range(2)]
    ).astype(jnp.int32)
    pair_order = jnp.stack(
        [(my_row ^ r) * chips + (my_chip ^ k) for k in range(chips) for r in range(rows)] + [my_core]
    ).astype(jnp.int32)

    def gather_update(value):
        return over_cores(over_chips([jnp.concatenate(over_rows(value), 0)]))

    first, second = pick_residual(block_index, residual_t)
    first = from_owner(first.astype(f16), owners[0])
    local, first_features, second_block = pick_features(
        block_index,
        block_index.T,
        (owners[0] == owners[1]).astype(jnp.int32)[None],
        features_t,
        second,
    )
    first = over_cores(over_chips([first]))
    first_features = over_cores(over_chips([from_owner(first_features, owners[0])]))
    second_block = over_cores(over_chips([from_owner(second_block, owners[1])]))
    first = [piece.astype(f32) for piece in first]
    update = first_update(col_order, first, block_inverse, 0)
    update = gather_update(update)
    width = features.shape[1]
    operator, base = second_operator(col_order, first_features, second_block, block_inverse, 1, width, scale)
    first_kernel = block_kernel(col_order, first_features, local, scale, "first_kernel")
    second_kernel = block_kernel(col_order, second_block, local, scale, "second_kernel")
    scalars = jnp.stack([my_col, my_row == owners[0], my_row == owners[1]]).astype(jnp.int32)
    later = gather_update(second_update(pair_order, update, operator, base))
    residual_t, coeffs_t = apply_update(
        scalars, pair_order, update, first_kernel, block_index, 0, residual_t, coeffs_t, "first_apply"
    )
    residual_t, coeffs_t = apply_update(
        scalars, pair_order, later, second_kernel, block_index, 1, residual_t, coeffs_t, "second_apply"
    )
    return (coeffs_t.T, residual_t.T)


def from_root(value, axis, source):
    kept = jnp.where(lax.axis_index(axis) == source, value, 0).astype(value.dtype)
    return lax.psum(kept, axis)


def per_device_plain(features, residual, coeffs, block_inverse, block_index, owners):
    frame_count = features.shape[0]
    feature_width = features.shape[1]
    per_col = block_index.shape[1]
    row_block = min(512, frame_count)
    exponent = -1.0 / feature_width
    my_row = lax.axis_index("rows")
    my_col = lax.axis_index("cols")
    squares = jnp.sum(jnp.square(features.astype(jnp.float32)), axis=1)
    feature_blocks = features.reshape(frame_count // row_block, row_block, feature_width)
    norm_blocks = squares.reshape(frame_count // row_block, row_block)
    for step_id in range(block_index.shape[0]):
        chosen_rows = block_index[step_id]
        owner_row = owners[step_id]
        mine_feat = jnp.take(features, chosen_rows, axis=0)
        mine_res = jnp.take(residual, chosen_rows, axis=0)
        row_piece = from_root(mine_feat, "rows", owner_row)
        chosen = lax.all_gather(row_piece, "cols", axis=0, tiled=True)
        res_piece = from_root(mine_res, "rows", owner_row)
        picked_res = lax.all_gather(res_piece, "cols", axis=0, tiled=True)
        my_update = jnp.dot(
            block_inverse[step_id],
            picked_res,
            precision=lax.Precision.HIGHEST,
            preferred_element_type=jnp.float32,
        ).astype(jnp.bfloat16)
        update = lax.all_gather(my_update, ("rows", "cols"), axis=0, tiled=True)
        chosen_norms = jnp.sum(jnp.square(chosen.astype(jnp.float32)), axis=1)

        def kernel_rows(operands):
            block_rows, block_norms = operands
            inner = lax.dot_general(
                block_rows, chosen, (((1,), (1,)), ((), ())), preferred_element_type=jnp.float32
            )
            distance = block_norms[:, None] + chosen_norms[None, :] - 2.0 * inner
            kernel = jnp.exp(distance * exponent).astype(jnp.bfloat16)
            return jnp.dot(kernel, update, preferred_element_type=jnp.float32)

        change = lax.map(kernel_rows, (feature_blocks, norm_blocks)).reshape(frame_count, -1)
        residual = residual - change
        is_owner = jnp.where(my_row == owner_row, 1.0, 0.0).astype(jnp.float32)
        mine_update = (
            lax.dynamic_slice_in_dim(update, my_col * per_col, per_col, 0).astype(jnp.float32)
            * is_owner
        )
        residual = residual.at[chosen_rows].add(-penalty * mine_update)
        coeffs = coeffs.at[chosen_rows].add(mine_update)
    return (coeffs, residual)


def power_of_two(value):
    return value & (value - 1) == 0


def solution(mesh):
    rows, cols = mesh.shape["rows"], mesh.shape["cols"]
    in_specs = (
        P(("rows", "cols"), None),
        P(("rows", "cols"), None),
        P(("rows", "cols"), None),
        P(None, ("rows", "cols"), None),
        P(None, "cols"),
        P(),
    )
    out_specs = (P(("rows", "cols"), None), P(("rows", "cols"), None))

    def per_device(features, residual, coeffs, block_inverse, block_index, owners):
        fits = (
            power_of_two(rows)
            and power_of_two(cols)
            and 2 <= rows <= 8
            and 2 <= cols <= 16
            and block_index.shape[0] == 2
            and block_index.shape[1] % LANES == 0
            and 2 * block_inverse.shape[1] == LANES
            and features.shape[0] % 512 == 0
        )
        args = (features, residual, coeffs, block_inverse, block_index, owners)
        return per_device_pieces(rows, cols, *args) if fits else per_device_plain(*args)

    return jax.shard_map(
        per_device, mesh=mesh, in_specs=in_specs, out_specs=out_specs, check_vma=False
    )
```

```python
import jax
import jax.numpy as jnp
from jax import lax
from jax.experimental import pallas as pl
from jax.experimental.pallas import tpu as pltpu
from jax.sharding import PartitionSpec as P


penalty = 0.5
LANES = 128
VMEM = pltpu.MemorySpace.VMEM
SMEM = pltpu.MemorySpace.SMEM
f32 = jnp.float32
bf16 = jnp.bfloat16
f16 = jnp.float16
MM = dict(preferred_element_type=f32)


def up(value, unit):
    return -(-value // unit) * unit


def params(megabytes=20):
    return pltpu.CompilerParams(vmem_limit_bytes=megabytes * 1024 * 1024)


def split(value, parts):
    pieces = []
    for _ in range(parts - 1):
        high = value.astype(bf16)
        pieces.append(high)
        value = value - high.astype(f32)
    pieces.append(value.astype(bf16))
    return pieces


def matmul(a, b):
    return lax.dot_general(a, b, (((1,), (0,)), ((), ())), **MM)


def matmul_nt(a, b):
    return lax.dot_general(a, b, (((1,), (1,)), ((), ())), **MM)


def one_hot(frames, index_row):
    rows = lax.broadcasted_iota(jnp.int32, (frames, index_row.shape[1]), 0)
    return jnp.where(rows == index_row, 1.0, 0.0).astype(bf16)


def turn(row):
    square = jnp.broadcast_to(row.astype(f32), (LANES, row.shape[1]))
    return jnp.transpose(square)[:, 0:1].astype(jnp.int32)


def padded(value, rows):
    return jnp.pad(value, ((0, rows - value.shape[0]), (0, 0)))


vmem = pl.BlockSpec(memory_space=VMEM)
smem = pl.BlockSpec(memory_space=SMEM)


def pick_residual(index, residual_t):
    outputs, frames = residual_t.shape
    rows = up(outputs, 16)
    picks = index.shape[1]

    def body(index_ref, residual_ref, first_ref):
        high, low = split(padded(residual_ref[...], rows), 2)
        first = matmul(jnp.concatenate([high, low], 0), one_hot(frames, index_ref[0:1, :]))
        first_ref[...] = first[:rows] + first[rows:]

    return pl.pallas_call(
        body,
        in_specs=[vmem, vmem],
        out_specs=vmem,
        out_shape=jax.ShapeDtypeStruct((rows, picks), f32),
        compiler_params=params(),
        name="pick_residual",
    )(index, residual_t)


def norm_rows(squares, kinds):
    width = squares.shape[1]
    norm = split(-0.5 * squares, 3)
    ones = jnp.ones((3, width), bf16)
    zeros = jnp.zeros((6, width), bf16)
    norm = jnp.concatenate(norm, 0)
    pieces = []
    for kind in kinds:
        if kind == 0:
            pieces.append(zeros)
        elif kind == 1:
            pieces.append(jnp.concatenate([norm, ones], 0))
        else:
            pieces.append(jnp.concatenate([ones, norm], 0))
    return jnp.concatenate(pieces, 0)


def pick_features(owners, index, features_t, residual_t):
    width, frames = features_t.shape
    outputs = residual_t.shape[0]
    depth = up(width + 20, 16)
    picks = index.shape[1]
    rows = up(outputs, 16)
    tail = depth - width

    def body(owners_ref, index_ref, features_ref, residual_ref, local_ref, first_ref, second_ref):
        features = features_ref[...]
        hot = one_hot(frames, index_ref[0:1, :])
        picked = matmul(features, hot)
        picked_squares = jnp.sum(picked * picked, axis=0, keepdims=True)
        first_ref[0:width, :] = picked.astype(bf16)
        rest = jnp.zeros((tail - 18, picks), bf16)
        first_ref[width:depth, :] = jnp.concatenate([norm_rows(picked_squares, (2, 0, 1)), rest], 0)

        hot = one_hot(frames, index_ref[1:2, :])
        picked = matmul(features, hot)
        picked_squares = jnp.sum(picked * picked, axis=0, keepdims=True)
        second_ref[0:width, :] = picked.astype(bf16)
        places = lax.broadcasted_iota(jnp.int32, (picks, picks), 0) + 1
        meet = jnp.where(turn(index_ref[0:1, :]) == index_ref[1:2, :], places, 0)
        place = jnp.max(meet, axis=0, keepdims=True)
        place = jnp.where(owners_ref[0] == owners_ref[1], place, 0)
        place = jnp.concatenate([place // LANES, place % LANES], 0).astype(f32).astype(bf16)
        rest = jnp.zeros((tail - 20, picks), bf16)
        second_ref[width:depth, :] = jnp.concatenate([norm_rows(picked_squares, (0, 2, 2)), place, rest], 0)
        high, low = split(padded(residual_ref[...], rows), 2)
        second_ref[depth:, :] = matmul(jnp.concatenate([high, low], 0), hot).astype(bf16)

        wide = features.astype(f32)
        squares = jnp.sum(wide * wide, axis=0, keepdims=True)
        local_ref[0:width, :] = features
        rest = jnp.zeros((tail - 18, frames), bf16)
        local_ref[width:depth, :] = jnp.concatenate([norm_rows(squares, (1, 1, 0)), rest], 0)

    return pl.pallas_call(
        body,
        in_specs=[smem, vmem, vmem, vmem],
        out_specs=(vmem, vmem, vmem),
        out_shape=(
            jax.ShapeDtypeStruct((depth, frames), bf16),
            jax.ShapeDtypeStruct((depth, picks), bf16),
            jax.ShapeDtypeStruct((depth + 2 * rows, picks), bf16),
        ),
        compiler_params=params(),
        name="pick_features",
    )(owners, index, features_t, residual_t)


def lane_start(value, unit):
    return pl.ds(pl.multiple_of(value * unit, unit), unit)


def piece_col(piece):
    mine = lax.axis_index("cols")
    return ((mine // 2) ^ (piece // 2)) * 2 + ((mine % 2) ^ (piece % 2))


def fold(update):
    half = update.shape[0] // 2
    return jnp.concatenate([update[:half], update[half:]], 1).astype(bf16)


def stack_inverse(inverse_ref, picks, stacked):
    for k in range(stacked.shape[1] // picks):
        high, low = split(inverse_ref[0, :, lane_start(piece_col(k), picks)], 2)
        stacked[:, k * picks : (k + 1) * picks] = jnp.concatenate([high, low], 0)


def first_update(picked, inverse, step, picks):
    rows, block = picked.shape
    mine = inverse.shape[1]

    def body(inverse_ref, picked_ref, out_ref, stacked):
        stack_inverse(inverse_ref, picks, stacked)
        product = matmul_nt(jnp.concatenate(split(picked_ref[...], 2), 0), stacked[...])
        product = product[:rows] + product[rows:]
        out_ref[...] = fold(product[:, :mine] + product[:, mine:])

    return pl.pallas_call(
        body,
        grid=(1,),
        in_specs=[pl.BlockSpec((1, mine, block), lambda i: (step, 0, 0)), vmem],
        out_specs=vmem,
        out_shape=jax.ShapeDtypeStruct((rows // 2, 2 * mine), bf16),
        scratch_shapes=[pltpu.VMEM((2 * mine, block), bf16)],
        compiler_params=params(),
        name="first_update",
    )(inverse, picked)


def second_operator(first, second, inverse, step, width, scale):
    depth, picks = first[0].shape
    count = len(first)
    block = picks * count
    mine = inverse.shape[1]
    rows = (second[0].shape[0] - depth) // 2
    wide = 2 * picks

    def body(inverse_ref, *refs):
        first_ref, second_ref = refs[:count], refs[count : 2 * count]
        operator_ref, base_ref, turned, stacked, kernel, meet = refs[2 * count :]
        stack_inverse(inverse_ref, picks, stacked)
        for k in range(count):
            turned[k * picks : (k + 1) * picks, :] = jnp.transpose(second_ref[k][0:depth, :])
        base = jnp.zeros((2 * rows, 2 * mine), f32)
        lanes = lax.broadcasted_iota(jnp.int32, (picks, picks), 1) + 1
        for k in range(count):
            base = base + matmul_nt(second_ref[k][depth:, :], stacked[:, k * picks : (k + 1) * picks])
            place = turned[k * picks : (k + 1) * picks, width + 18 : width + 20].astype(f32)
            place = (place[:, 0:1] * LANES + place[:, 1:2]).astype(jnp.int32)
            meet[k * picks : (k + 1) * picks, :] = jnp.where(place == lanes, penalty, 0.0).astype(bf16)
        for n in range(0, count, 2):
            columns = jnp.concatenate([first_ref[n][...], first_ref[n + 1][...]], 1)
            for k in range(count):
                here = slice(k * picks, (k + 1) * picks)
                inner = matmul(turned[here, :], columns)
                kernel[here, :] = jnp.exp2(inner * scale).astype(bf16)
            for k in (n, n + 1):
                here = slice(k * picks, (k + 1) * picks)
                there = slice((k - n) * picks, (k - n + 1) * picks)
                kernel[here, there] = kernel[here, there] + meet[here, :]
            product = matmul(stacked[...], kernel[...])
            high, low = split(product[0:mine, :] + product[mine:, :], 2)
            operator_ref[0:mine, n * picks : n * picks + wide] = high
            operator_ref[mine:, n * picks : n * picks + wide] = low
        base = base[:rows] + base[rows:]
        base_ref[...] = base[:, :mine] + base[:, mine:]

    flops = 2 * block * block * (depth + 2 * mine)
    return pl.pallas_call(
        body,
        grid=(1,),
        in_specs=[pl.BlockSpec((1, mine, block), lambda i: (step, 0, 0))] + [vmem] * (2 * count),
        out_specs=(vmem, vmem),
        out_shape=(
            jax.ShapeDtypeStruct((2 * mine, block), bf16),
            jax.ShapeDtypeStruct((rows, mine), f32),
        ),
        scratch_shapes=[
            pltpu.VMEM((block, depth), bf16),
            pltpu.VMEM((2 * mine, block), bf16),
            pltpu.VMEM((block, wide), bf16),
            pltpu.VMEM((block, picks), bf16),
        ],
        cost_estimate=pl.CostEstimate(flops=flops, transcendentals=block * block, bytes_accessed=10**7),
        compiler_params=params(),
        name="second_operator",
    )(inverse, *first, *second)


def block_kernel(pieces, local, scale):
    depth, frames = local.shape
    picks = pieces[0].shape[1]
    count = len(pieces)
    block = picks * count
    tile = min(512, frames)

    def body(local_ref, *refs):
        pieces_ref, out_ref, turned = refs[:count], refs[-2], refs[-1]

        @pl.when(pl.program_id(0) == 0)
        def _():
            for k in range(count):
                turned[k * picks : (k + 1) * picks, :] = jnp.transpose(pieces_ref[k][0:depth, :])

        for k in range(count):
            here = slice(k * picks, (k + 1) * picks)
            inner = matmul(turned[here, :], local_ref[...])
            out_ref[here, :] = jnp.exp2(inner * scale).astype(bf16)

    return pl.pallas_call(
        body,
        grid=(frames // tile,),
        in_specs=[pl.BlockSpec((depth, tile), lambda i: (0, i))] + [vmem] * count,
        out_specs=pl.BlockSpec((block, tile), lambda i: (0, i)),
        out_shape=jax.ShapeDtypeStruct((block, frames), bf16),
        scratch_shapes=[pltpu.VMEM((block, depth), bf16)],
        cost_estimate=pl.CostEstimate(
            flops=2 * block * frames * depth, transcendentals=block * frames, bytes_accessed=10**7
        ),
        compiler_params=params(),
    )(local, *pieces)


def unfold(pieces_ref, parts, picks, canon):
    half, width = pieces_ref[0].shape[0] // parts, pieces_ref[0].shape[1]
    mine = width // 2
    count = len(pieces_ref)
    lanes = lax.broadcasted_iota(jnp.int32, (half, width), 1)
    low = lanes < mine
    row, col = lax.axis_index("rows"), lax.axis_index("cols")
    core = col % 2
    for k in range(0, count, 2):
        for r in range(parts):
            here = pieces_ref[k][r * half : (r + 1) * half, :].astype(f32)
            other = pieces_ref[k + 1][r * half : (r + 1) * half, :].astype(f32)
            a = jnp.where(core == 0, here, other)
            b = jnp.where(core == 0, other, here)
            upper = jnp.where(low, a, pltpu.roll(b, mine, 1))
            lower = jnp.where(low, pltpu.roll(a, mine, 1), b)
            pair = (row ^ r) * (count // 2) + ((col // 2) ^ (k // 2))
            from_col = pair * width // picks
            place = ((from_col // 2) ^ (col // 2)) * 2 + ((from_col % 2) ^ core)
            place = pl.ds(pl.multiple_of(place * picks + pair * width % picks, width), width)
            canon[0:half, place] = upper.astype(bf16)
            canon[half:, place] = lower.astype(bf16)


def second_update(pieces, operator, base, picks):
    rows, mine = base.shape
    block = operator.shape[1]
    count = len(pieces)

    def body(operator_ref, base_ref, *refs):
        pieces_ref, out_ref, canon = refs[:count], refs[-2], refs[-1]
        unfold(pieces_ref, pieces[0].shape[0] * 2 // rows, picks, canon)
        product = matmul_nt(canon[...], operator_ref[...])
        out_ref[...] = fold(base_ref[...] - (product[:, :mine] + product[:, mine:]))

    return pl.pallas_call(
        body,
        in_specs=[vmem] * (2 + count),
        out_specs=vmem,
        out_shape=jax.ShapeDtypeStruct((rows // 2, 2 * mine), bf16),
        scratch_shapes=[pltpu.VMEM((rows, block), bf16)],
        compiler_params=params(),
        name="second_update",
    )(operator, base, *pieces)


def apply_update(owners, pieces, kernel, index, step, residual_t, coeffs_t):
    outputs, frames = residual_t.shape
    block = kernel.shape[0]
    picks = index.shape[1]
    count = len(pieces)
    rows = up(outputs, 16)
    tile = min(512, frames)

    def body(owners_ref, index_ref, kernel_ref, residual_ref, coeffs_ref, *refs):
        pieces_ref = refs[:count]
        new_residual_ref, new_coeffs_ref, canon, own = refs[count:]
        here = pl.program_id(0)

        @pl.when(here == 0)
        def _():
            unfold(pieces_ref, pieces[0].shape[0] * 2 // rows, picks, canon)
            mine = canon[:, 0:picks]
            own[...] = jnp.where(lax.axis_index("rows") == owners_ref[step], mine, jnp.zeros_like(mine))

        change = matmul(canon[...], kernel_ref[...])
        frame = lax.broadcasted_iota(jnp.int32, (tile, picks), 0) + here * tile
        hot = jnp.where(frame == index_ref[step : step + 1, :], 1.0, 0.0).astype(bf16)
        put = matmul_nt(own[...], hot)
        new_residual_ref[...] = residual_ref[...] - (change + penalty * put)[:outputs]
        new_coeffs_ref[...] = coeffs_ref[...] + put[:outputs]

    strip = pl.BlockSpec((outputs, tile), lambda i: (0, i))
    return pl.pallas_call(
        body,
        grid=(frames // tile,),
        in_specs=[smem, vmem, pl.BlockSpec((block, tile), lambda i: (0, i)), strip, strip] + [vmem] * count,
        out_specs=(strip, strip),
        out_shape=(
            jax.ShapeDtypeStruct((outputs, frames), f32),
            jax.ShapeDtypeStruct((outputs, frames), f32),
        ),
        scratch_shapes=[pltpu.VMEM((rows, block), bf16), pltpu.VMEM((rows, picks), bf16)],
        cost_estimate=pl.CostEstimate(
            flops=2 * rows * block * frames, transcendentals=0, bytes_accessed=2 * block * frames
        ),
        compiler_params=params(),
    )(owners, index, kernel, residual_t, coeffs_t, *pieces)


class Sender:
    def __init__(self, rows, cols):
        self.rows, self.cols, self.chips = rows, cols, cols // 2
        self.row = lax.axis_index("rows")

    def send(self, value, row=None, chip_step=0, core_step=0):
        pairs = []
        for i in range(self.rows * self.cols):
            at, col = i // self.cols, i % self.cols
            to = at if row is None else row(at)
            if to is None:
                continue
            col = ((col // 2) ^ chip_step) * 2 + ((col % 2) ^ core_step)
            pairs.append((i, to * self.cols + col))
        return lax.ppermute(value, ("rows", "cols"), pairs)

    def doubling(self, value, owner):
        step = 1
        while step < self.rows:
            other = self.send(value, row=lambda at, step=step: at ^ step)
            value = jnp.where(((owner ^ self.row) & step) != 0, other, value)
            step *= 2
        return value

    def along(self, value, owner):
        count, row = self.rows, self.row
        half = count // 2
        lower = row < half
        moves = []
        for s in range(half - 1):
            moves.append((s, {s: s + 1, count - 1 - s: count - 2 - s}))
        moves.append((None, {half - 1: half, half: half - 1}))
        for s in reversed(range(half - 1)):
            moves.append((~s, {s + 1: s, count - 2 - s: count - 1 - s}))
        for s, move in moves:
            other = self.send(value, row=move.get)
            if s is None:
                take = ((row == half - 1) & (owner >= half)) | ((row == half) & (owner < half))
            elif s >= 0:
                take = ((row == s + 1) & (owner <= s)) | ((row == count - 2 - s) & (owner >= count - 1 - s))
            else:
                s = ~s
                take = ((row == s) & (owner > s)) | ((row == count - 1 - s) & (owner < count - 1 - s))
            value = jnp.where(take, other, value)
        return value

    def over_rows(self, value):
        steps = sorted(range(1, self.rows), key=lambda k: -k)
        got = {k: self.send(value, row=lambda at, k=k: at ^ k) for k in steps}
        return [value] + [got[k] for k in range(1, self.rows)]

    def over_cols(self, value):
        found = []
        for k in range(self.chips):
            mine = value if k == 0 else self.send(value, chip_step=k)
            found += [mine, self.send(mine, core_step=1)]
        return found


def per_device_pieces(rows, cols, features, residual, coeffs, block_inverse, block_index, owners):
    scale = 2.0 / features.shape[1] * 1.4426950408889634
    sender = Sender(rows, cols)
    width, picks = features.shape[1], block_index.shape[1]
    features_t, residual_t, coeffs_t = features.T, residual.T, coeffs.T
    first = pick_residual(block_index, residual_t)
    first = sender.over_cols(sender.doubling(first.astype(f16), owners[0]))
    local, first_block, second_block = pick_features(owners, block_index, features_t, residual_t)
    first_block = sender.over_cols(sender.along(first_block, owners[0]))
    second_block = sender.over_cols(sender.along(second_block, owners[1]))
    update = first_update(jnp.concatenate(first, 1).astype(f32), block_inverse, 0, picks)
    update = sender.over_cols(jnp.concatenate(sender.over_rows(update), 0))
    first_kernel = block_kernel(first_block, local, scale)
    operator, base = second_operator(first_block, second_block, block_inverse, 1, width, scale)
    later = second_update(update, operator, base, picks)
    later = sender.over_cols(jnp.concatenate(sender.over_rows(later), 0))
    second_kernel = block_kernel(second_block, local, scale)
    residual_t, coeffs_t = apply_update(
        owners, update, first_kernel, block_index, 0, residual_t, coeffs_t
    )
    residual_t, coeffs_t = apply_update(
        owners, later, second_kernel, block_index, 1, residual_t, coeffs_t
    )
    return (coeffs_t.T, residual_t.T)


def from_root(value, axis, source):
    kept = jnp.where(lax.axis_index(axis) == source, value, 0).astype(value.dtype)
    return lax.psum(kept, axis)


def per_device_plain(features, residual, coeffs, block_inverse, block_index, owners):
    frame_count = features.shape[0]
    feature_width = features.shape[1]
    per_col = block_index.shape[1]
    row_block = min(512, frame_count)
    exponent = -1.0 / feature_width
    my_row = lax.axis_index("rows")
    my_col = lax.axis_index("cols")
    squares = jnp.sum(jnp.square(features.astype(jnp.float32)), axis=1)
    feature_blocks = features.reshape(frame_count // row_block, row_block, feature_width)
    norm_blocks = squares.reshape(frame_count // row_block, row_block)
    for step_id in range(block_index.shape[0]):
        chosen_rows = block_index[step_id]
        owner_row = owners[step_id]
        mine_feat = jnp.take(features, chosen_rows, axis=0)
        mine_res = jnp.take(residual, chosen_rows, axis=0)
        row_piece = from_root(mine_feat, "rows", owner_row)
        chosen = lax.all_gather(row_piece, "cols", axis=0, tiled=True)
        res_piece = from_root(mine_res, "rows", owner_row)
        picked_res = lax.all_gather(res_piece, "cols", axis=0, tiled=True)
        my_update = jnp.dot(
            block_inverse[step_id],
            picked_res,
            precision=lax.Precision.HIGHEST,
            preferred_element_type=jnp.float32,
        ).astype(jnp.bfloat16)
        update = lax.all_gather(my_update, ("rows", "cols"), axis=0, tiled=True)
        chosen_norms = jnp.sum(jnp.square(chosen.astype(jnp.float32)), axis=1)

        def kernel_rows(operands):
            block_rows, block_norms = operands
            inner = lax.dot_general(
                block_rows, chosen, (((1,), (1,)), ((), ())), preferred_element_type=jnp.float32
            )
            distance = block_norms[:, None] + chosen_norms[None, :] - 2.0 * inner
            kernel = jnp.exp(distance * exponent).astype(jnp.bfloat16)
            return jnp.dot(kernel, update, preferred_element_type=jnp.float32)

        change = lax.map(kernel_rows, (feature_blocks, norm_blocks)).reshape(frame_count, -1)
        residual = residual - change
        is_owner = jnp.where(my_row == owner_row, 1.0, 0.0).astype(jnp.float32)
        mine_update = (
            lax.dynamic_slice_in_dim(update, my_col * per_col, per_col, 0).astype(jnp.float32)
            * is_owner
        )
        residual = residual.at[chosen_rows].add(-penalty * mine_update)
        coeffs = coeffs.at[chosen_rows].add(mine_update)
    return (coeffs, residual)


def power_of_two(value):
    return value & (value - 1) == 0


def solution(mesh):
    rows, cols = mesh.shape["rows"], mesh.shape["cols"]
    in_specs = (
        P(("rows", "cols"), None),
        P(("rows", "cols"), None),
        P(("rows", "cols"), None),
        P(None, ("rows", "cols"), None),
        P(None, "cols"),
        P(),
    )
    out_specs = (P(("rows", "cols"), None), P(("rows", "cols"), None))

    def per_device(features, residual, coeffs, block_inverse, block_index, owners):
        args = (features, residual, coeffs, block_inverse, block_index, owners)
        return per_device_pieces(rows, cols, *args) if fits(*args) else per_device_plain(*args)

    def fits(features, residual, coeffs, block_inverse, block_index, owners):
        return (
            small
            and block_index.shape[0] == 2
            and block_index.shape[1] % LANES == 0
            and 2 * block_inverse.shape[1] == LANES
            and features.shape[0] % 512 == 0
        )

    small = power_of_two(rows) and power_of_two(cols) and 2 <= rows <= 8 and 4 <= cols <= 16
    return jax.shard_map(
        per_device, mesh=mesh, in_specs=in_specs, out_specs=out_specs, check_vma=False
    )
```

```python
import jax
import jax.numpy as jnp
from jax import lax
from jax.experimental import pallas as pl
from jax.experimental.pallas import tpu as pltpu
from jax.sharding import PartitionSpec as P


penalty = 0.5
LANES = 128
VMEM = pltpu.MemorySpace.VMEM
SMEM = pltpu.MemorySpace.SMEM
f32 = jnp.float32
bf16 = jnp.bfloat16
f16 = jnp.float16
MM = dict(preferred_element_type=f32)


def up(value, unit):
    return -(-value // unit) * unit


def params(megabytes=20):
    return pltpu.CompilerParams(vmem_limit_bytes=megabytes * 1024 * 1024)


def split(value, parts):
    pieces = []
    for _ in range(parts - 1):
        high = value.astype(bf16)
        pieces.append(high)
        value = value - high.astype(f32)
    pieces.append(value.astype(bf16))
    return pieces


def matmul(a, b):
    return lax.dot_general(a, b, (((1,), (0,)), ((), ())), **MM)


def matmul_nt(a, b):
    return lax.dot_general(a, b, (((1,), (1,)), ((), ())), **MM)


def one_hot(frames, index_row):
    rows = lax.broadcasted_iota(jnp.int32, (frames, index_row.shape[1]), 0)
    return jnp.where(rows == index_row, 1.0, 0.0).astype(bf16)


def turn(row):
    square = jnp.broadcast_to(row.astype(f32), (LANES, row.shape[1]))
    return jnp.transpose(square)[:, 0:1].astype(jnp.int32)


def padded(value, rows):
    return jnp.pad(value, ((0, rows - value.shape[0]), (0, 0)))


vmem = pl.BlockSpec(memory_space=VMEM)
smem = pl.BlockSpec(memory_space=SMEM)


def pick_residual(index, residual_t):
    outputs, frames = residual_t.shape
    rows = up(outputs, 16)
    steps, picks = index.shape

    def body(index_ref, residual_ref, *out_ref):
        both = jnp.concatenate(split(padded(residual_ref[...], rows), 2), 0)
        for step in range(steps):
            found = matmul(both, one_hot(frames, index_ref[step : step + 1, :]))
            out_ref[step][...] = found[:rows] + found[rows:]

    return pl.pallas_call(
        body,
        in_specs=[vmem, vmem],
        out_specs=(vmem,) * steps,
        out_shape=(jax.ShapeDtypeStruct((rows, picks), f32),) * steps,
        compiler_params=params(),
        name="pick_residual",
    )(index, residual_t)


def norm_rows(squares, kinds):
    width = squares.shape[1]
    norm = split(-0.5 * squares, 3)
    ones = jnp.ones((3, width), bf16)
    zeros = jnp.zeros((6, width), bf16)
    norm = jnp.concatenate(norm, 0)
    pieces = []
    for kind in kinds:
        if kind == 0:
            pieces.append(zeros)
        elif kind == 1:
            pieces.append(jnp.concatenate([norm, ones], 0))
        else:
            pieces.append(jnp.concatenate([ones, norm], 0))
    return jnp.concatenate(pieces, 0)


def pick_features(owners, index, features_t, rules):
    width, frames = features_t.shape
    depth = up(width + 18, 16)
    steps, picks = index.shape
    kinds = ((2, 0, 1), (0, 2, 2))

    def body(owners_ref, index_ref, features_ref, *out_ref):
        features = features_ref[...]
        rest = jnp.zeros((depth - width - 18, picks), bf16)
        for step in range(steps):
            picked = matmul(features, one_hot(frames, index_ref[step : step + 1, :]))
            squares = jnp.sum(picked * picked, axis=0, keepdims=True)
            out_ref[step][0:width, :] = picked.astype(bf16)
            out_ref[step][width:depth, :] = jnp.concatenate([norm_rows(squares, kinds[step]), rest], 0)
        row = lax.axis_index("rows")
        for (step, rule), take_ref in zip(rules, out_ref[steps:]):
            take = jnp.where(rule(row, owners_ref[step]), 1.0, 0.0)
            take_ref[...] = jnp.full(take_ref.shape, take, f32)

    return pl.pallas_call(
        body,
        in_specs=[smem, vmem, vmem],
        out_specs=(vmem,) * (steps + len(rules)),
        out_shape=(jax.ShapeDtypeStruct((depth, picks), bf16),) * steps
        + (jax.ShapeDtypeStruct((1, picks), f32),) * len(rules),
        compiler_params=params(),
        name="pick_features",
    )(owners, index, features_t)


def lane_start(value, unit):
    return pl.ds(pl.multiple_of(value * unit, unit), unit)


def piece_col(piece):
    mine = lax.axis_index("cols")
    return ((mine // 2) ^ (piece // 2)) * 2 + ((mine % 2) ^ (piece % 2))


def fold(update):
    half = update.shape[0] // 2
    return jnp.concatenate([update[:half], update[half:]], 1).astype(bf16)


def prepare(features_t, inverse, picks):
    width, frames = features_t.shape
    depth = up(width + 18, 16)
    steps, mine, block = inverse.shape

    def body(features_ref, inverse_ref, local_ref, *stacked_ref):
        features = features_ref[...]
        wide = features.astype(f32)
        squares = jnp.sum(wide * wide, axis=0, keepdims=True)
        local_ref[0:width, :] = features
        rest = jnp.zeros((depth - width - 18, frames), bf16)
        local_ref[width:depth, :] = jnp.concatenate([norm_rows(squares, (1, 1, 0)), rest], 0)
        for step in range(steps):
            for k in range(block // picks):
                high, low = split(inverse_ref[step, :, lane_start(piece_col(k), picks)], 2)
                stacked_ref[step][:, k * picks : (k + 1) * picks] = jnp.concatenate([high, low], 0)

    return pl.pallas_call(
        body,
        in_specs=[vmem, vmem],
        out_specs=(vmem,) * (1 + steps),
        out_shape=(jax.ShapeDtypeStruct((depth, frames), bf16),)
        + (jax.ShapeDtypeStruct((2 * mine, block), bf16),) * steps,
        compiler_params=params(),
        name="prepare",
    )(features_t, inverse)


def block_update(picked, stacked, scaled):
    rows, _ = picked.shape
    mine = stacked.shape[0] // 2

    def body(stacked_ref, picked_ref, out_ref):
        product = matmul_nt(jnp.concatenate(split(picked_ref[...], 2), 0), stacked_ref[...])
        product = product[:rows] + product[rows:]
        out_ref[...] = fold((product[:, :mine] + product[:, mine:]) * scaled)

    return pl.pallas_call(
        body,
        in_specs=[vmem, vmem],
        out_specs=vmem,
        out_shape=jax.ShapeDtypeStruct((rows // 2, 2 * mine), bf16),
        compiler_params=params(),
    )(stacked, picked)


def meeting_kernel(owners, index, pieces, second, scale):
    depth, picks = second.shape
    count = len(pieces)

    def body(owners_ref, index_ref, second_ref, *refs):
        pieces_ref, out_ref = refs[:count], refs[-1]
        for k in range(count):
            inner = matmul(jnp.transpose(pieces_ref[k][...]), second_ref[...])
            kernel = jnp.exp2(inner * scale).astype(bf16)
            if k == 0:
                same = turn(index_ref[0:1, :]) == index_ref[1:2, :]
                bonus = jnp.where(owners_ref[0] == owners_ref[1], penalty, 0.0)
                kernel = kernel + jnp.where(same, bonus, 0.0).astype(bf16)
            out_ref[k * picks : (k + 1) * picks, :] = kernel

    return pl.pallas_call(
        body,
        in_specs=[smem, vmem, vmem] + [vmem] * count,
        out_specs=vmem,
        out_shape=jax.ShapeDtypeStruct((count * picks, picks), bf16),
        cost_estimate=pl.CostEstimate(
            flops=2 * count * picks * picks * depth, transcendentals=count * picks * picks, bytes_accessed=10**6
        ),
        compiler_params=params(),
        name="meeting_kernel",
    )(owners, index, second, *pieces)


def advance(kernel, before, pieces, scaled):
    rows, picks = before.shape
    block = kernel.shape[0]
    count = len(pieces)

    def body(kernel_ref, before_ref, *refs):
        pieces_ref, out_ref, canon = refs[:count], refs[-2], refs[-1]
        unfold(pieces_ref, pieces[0].shape[0] * 2 // rows, picks, canon)
        out_ref[...] = (before_ref[...] - matmul(canon[...], kernel_ref[...])) * scaled

    return pl.pallas_call(
        body,
        in_specs=[vmem] * (2 + count),
        out_specs=vmem,
        out_shape=jax.ShapeDtypeStruct((rows, picks), f32),
        scratch_shapes=[pltpu.VMEM((rows, block), bf16)],
        compiler_params=params(),
        name="advance",
    )(kernel, before, *pieces)


def block_kernel(pieces, local, scale):
    depth, frames = local.shape
    picks = pieces[0].shape[1]
    count = len(pieces)
    block = picks * count
    tile = min(512, frames)

    def body(local_ref, *refs):
        pieces_ref, out_ref, turned = refs[:count], refs[-2], refs[-1]

        @pl.when(pl.program_id(0) == 0)
        def _():
            for k in range(count):
                turned[k * picks : (k + 1) * picks, :] = jnp.transpose(pieces_ref[k][0:depth, :])

        for k in range(count):
            here = slice(k * picks, (k + 1) * picks)
            inner = matmul(turned[here, :], local_ref[...])
            out_ref[here, :] = jnp.exp2(inner * scale).astype(bf16)

    return pl.pallas_call(
        body,
        grid=(frames // tile,),
        in_specs=[pl.BlockSpec((depth, tile), lambda i: (0, i))] + [vmem] * count,
        out_specs=pl.BlockSpec((block, tile), lambda i: (0, i)),
        out_shape=jax.ShapeDtypeStruct((block, frames), bf16),
        scratch_shapes=[pltpu.VMEM((block, depth), bf16)],
        cost_estimate=pl.CostEstimate(
            flops=2 * block * frames * depth, transcendentals=block * frames, bytes_accessed=10**7
        ),
        compiler_params=params(),
    )(local, *pieces)


def unfold(pieces_ref, parts, picks, canon):
    half, width = pieces_ref[0].shape[0] // parts, pieces_ref[0].shape[1]
    mine = width // 2
    count = len(pieces_ref)
    lanes = lax.broadcasted_iota(jnp.int32, (half, width), 1)
    low = lanes < mine
    row, col = lax.axis_index("rows"), lax.axis_index("cols")
    core = col % 2
    for k in range(0, count, 2):
        for r in range(parts):
            here = pieces_ref[k][r * half : (r + 1) * half, :].astype(f32)
            other = pieces_ref[k + 1][r * half : (r + 1) * half, :].astype(f32)
            a = jnp.where(core == 0, here, other)
            b = jnp.where(core == 0, other, here)
            upper = jnp.where(low, a, pltpu.roll(b, mine, 1))
            lower = jnp.where(low, pltpu.roll(a, mine, 1), b)
            pair = (row ^ r) * (count // 2) + ((col // 2) ^ (k // 2))
            from_col = pair * width // picks
            place = ((from_col // 2) ^ (col // 2)) * 2 + ((from_col % 2) ^ core)
            place = pl.ds(pl.multiple_of(place * picks + pair * width % picks, width), width)
            canon[0:half, place] = upper.astype(bf16)
            canon[half:, place] = lower.astype(bf16)


def apply_update(owners, pieces, kernel, index, step, residual_t, coeffs_t):
    outputs, frames = residual_t.shape
    block = kernel.shape[0]
    picks = index.shape[1]
    count = len(pieces)
    rows = up(outputs, 16)
    tile = min(512, frames)

    def body(owners_ref, index_ref, kernel_ref, residual_ref, coeffs_ref, *refs):
        pieces_ref = refs[:count]
        new_residual_ref, new_coeffs_ref, canon, own = refs[count:]
        here = pl.program_id(0)

        @pl.when(here == 0)
        def _():
            unfold(pieces_ref, pieces[0].shape[0] * 2 // rows, picks, canon)
            mine = canon[:, 0:picks]
            own[...] = jnp.where(lax.axis_index("rows") == owners_ref[step], mine, jnp.zeros_like(mine))

        change = matmul(canon[...], kernel_ref[...])
        frame = lax.broadcasted_iota(jnp.int32, (tile, picks), 0) + here * tile
        hot = jnp.where(frame == index_ref[step : step + 1, :], 1.0, 0.0).astype(bf16)
        put = matmul_nt(own[...], hot)
        new_residual_ref[...] = residual_ref[...] - (change + penalty * put)[:outputs]
        new_coeffs_ref[...] = coeffs_ref[...] + put[:outputs]

    strip = pl.BlockSpec((outputs, tile), lambda i: (0, i))
    return pl.pallas_call(
        body,
        grid=(frames // tile,),
        in_specs=[smem, vmem, pl.BlockSpec((block, tile), lambda i: (0, i)), strip, strip] + [vmem] * count,
        out_specs=(strip, strip),
        out_shape=(
            jax.ShapeDtypeStruct((outputs, frames), f32),
            jax.ShapeDtypeStruct((outputs, frames), f32),
        ),
        scratch_shapes=[pltpu.VMEM((rows, block), bf16), pltpu.VMEM((rows, picks), bf16)],
        cost_estimate=pl.CostEstimate(
            flops=2 * rows * block * frames, transcendentals=0, bytes_accessed=2 * block * frames
        ),
        compiler_params=params(),
    )(owners, index, kernel, residual_t, coeffs_t, *pieces)


class Sender:
    def __init__(self, rows, cols):
        self.rows, self.cols, self.chips = rows, cols, cols // 2

    def send(self, value, row=None, chip_step=0, core_step=0):
        pairs = []
        for i in range(self.rows * self.cols):
            at, col = i // self.cols, i % self.cols
            to = at if row is None else row(at)
            if to is None:
                continue
            col = ((col // 2) ^ chip_step) * 2 + ((col % 2) ^ core_step)
            pairs.append((i, to * self.cols + col))
        return lax.ppermute(value, ("rows", "cols"), pairs)

    def spread(self, value, moves, takes):
        for move, take in zip(moves, takes):
            other = self.send(value, row=move)
            value = jnp.where(take > 0.5, other, value)
        return value

    def over_rows(self, value):
        steps = sorted(range(1, self.rows), key=lambda k: -k)
        got = {k: self.send(value, row=lambda at, k=k: at ^ k) for k in steps}
        return [value] + [got[k] for k in range(1, self.rows)]

    def over_cores(self, values):
        return [side for v in values for side in (v, self.send(v, core_step=1))]

    def over_cols(self, value):
        values = [value] + [self.send(value, chip_step=k) for k in range(1, self.chips)]
        return self.over_cores(values)


def doubling(rows):
    steps = [1 << k for k in range(rows.bit_length() - 1)]
    moves = [lambda at, step=step: at ^ step for step in steps]
    rules = [lambda row, owner, step=step: ((row ^ owner) & step) != 0 for step in steps]
    return moves, rules


def per_device_pieces(rows, cols, features, residual, coeffs, block_inverse, block_index, owners):
    scale = 2.0 / features.shape[1] * 1.4426950408889634
    sender = Sender(rows, cols)
    picks = block_index.shape[1]
    moves, rules = doubling(rows)
    scaled = 2.0**-4 * (2048 / block_inverse.shape[2]) ** 2
    features_t, residual_t, coeffs_t = features.T, residual.T, coeffs.T
    first, second = pick_residual(block_index, residual_t)
    first_block, second_block, *takes = pick_features(
        owners, block_index, features_t, [(step, rule) for step in range(2) for rule in rules]
    )
    local, *stacked = prepare(features_t, block_inverse, picks)
    first = sender.over_cols(sender.spread(first.astype(f16), moves, takes))
    first_block = sender.over_cols(sender.spread(first_block, moves, takes))
    second = sender.spread(second.astype(f16), moves, takes[len(rules) :]).astype(f32)
    second_block = sender.spread(second_block, moves, takes[len(rules) :])
    update = block_update(jnp.concatenate(first, 1).astype(f32), stacked[0], 1.0)
    update = sender.over_cols(jnp.concatenate(sender.over_rows(update), 0))
    meeting = meeting_kernel(owners, block_index, first_block, second_block, scale)
    second = sender.over_cols(advance(meeting, second, update, scaled).astype(f16))
    first_kernel = block_kernel(first_block, local, scale)
    later = block_update(jnp.concatenate(second, 1).astype(f32), stacked[1], 1.0 / scaled)
    later = sender.over_cols(jnp.concatenate(sender.over_rows(later), 0))
    second_block = sender.over_cols(second_block)
    second_kernel = block_kernel(second_block, local, scale)
    residual_t, coeffs_t = apply_update(
        owners, update, first_kernel, block_index, 0, residual_t, coeffs_t
    )
    residual_t, coeffs_t = apply_update(
        owners, later, second_kernel, block_index, 1, residual_t, coeffs_t
    )
    return (coeffs_t.T, residual_t.T)


def from_root(value, axis, source):
    kept = jnp.where(lax.axis_index(axis) == source, value, 0).astype(value.dtype)
    return lax.psum(kept, axis)


def per_device_plain(features, residual, coeffs, block_inverse, block_index, owners):
    frame_count = features.shape[0]
    feature_width = features.shape[1]
    per_col = block_index.shape[1]
    row_block = min(512, frame_count)
    exponent = -1.0 / feature_width
    my_row = lax.axis_index("rows")
    my_col = lax.axis_index("cols")
    squares = jnp.sum(jnp.square(features.astype(jnp.float32)), axis=1)
    feature_blocks = features.reshape(frame_count // row_block, row_block, feature_width)
    norm_blocks = squares.reshape(frame_count // row_block, row_block)
    for step_id in range(block_index.shape[0]):
        chosen_rows = block_index[step_id]
        owner_row = owners[step_id]
        mine_feat = jnp.take(features, chosen_rows, axis=0)
        mine_res = jnp.take(residual, chosen_rows, axis=0)
        row_piece = from_root(mine_feat, "rows", owner_row)
        chosen = lax.all_gather(row_piece, "cols", axis=0, tiled=True)
        res_piece = from_root(mine_res, "rows", owner_row)
        picked_res = lax.all_gather(res_piece, "cols", axis=0, tiled=True)
        my_update = jnp.dot(
            block_inverse[step_id],
            picked_res,
            precision=lax.Precision.HIGHEST,
            preferred_element_type=jnp.float32,
        ).astype(jnp.bfloat16)
        update = lax.all_gather(my_update, ("rows", "cols"), axis=0, tiled=True)
        chosen_norms = jnp.sum(jnp.square(chosen.astype(jnp.float32)), axis=1)

        def kernel_rows(operands):
            block_rows, block_norms = operands
            inner = lax.dot_general(
                block_rows, chosen, (((1,), (1,)), ((), ())), preferred_element_type=jnp.float32
            )
            distance = block_norms[:, None] + chosen_norms[None, :] - 2.0 * inner
            kernel = jnp.exp(distance * exponent).astype(jnp.bfloat16)
            return jnp.dot(kernel, update, preferred_element_type=jnp.float32)

        change = lax.map(kernel_rows, (feature_blocks, norm_blocks)).reshape(frame_count, -1)
        residual = residual - change
        is_owner = jnp.where(my_row == owner_row, 1.0, 0.0).astype(jnp.float32)
        mine_update = (
            lax.dynamic_slice_in_dim(update, my_col * per_col, per_col, 0).astype(jnp.float32)
            * is_owner
        )
        residual = residual.at[chosen_rows].add(-penalty * mine_update)
        coeffs = coeffs.at[chosen_rows].add(mine_update)
    return (coeffs, residual)


def power_of_two(value):
    return value & (value - 1) == 0


def solution(mesh):
    rows, cols = mesh.shape["rows"], mesh.shape["cols"]
    in_specs = (
        P(("rows", "cols"), None),
        P(("rows", "cols"), None),
        P(("rows", "cols"), None),
        P(None, ("rows", "cols"), None),
        P(None, "cols"),
        P(),
    )
    out_specs = (P(("rows", "cols"), None), P(("rows", "cols"), None))

    def per_device(features, residual, coeffs, block_inverse, block_index, owners):
        args = (features, residual, coeffs, block_inverse, block_index, owners)
        return per_device_pieces(rows, cols, *args) if fits(*args) else per_device_plain(*args)

    def fits(features, residual, coeffs, block_inverse, block_index, owners):
        return (
            small
            and block_index.shape[0] == 2
            and block_index.shape[1] % LANES == 0
            and 2 * block_inverse.shape[1] == LANES
            and features.shape[0] % 512 == 0
        )

    small = power_of_two(rows) and power_of_two(cols) and 2 <= rows <= 8 and 4 <= cols <= 16
    return jax.shard_map(
        per_device, mesh=mesh, in_specs=in_specs, out_specs=out_specs, check_vma=False
    )
```

```python
import math

import jax
import jax.numpy as jnp
from jax import lax
from jax.experimental import pallas as pl
from jax.experimental.pallas import tpu as pltpu
from jax.sharding import PartitionSpec as P


penalty = 0.5
LANES = 128
VMEM = pltpu.MemorySpace.VMEM
SMEM = pltpu.MemorySpace.SMEM
f32 = jnp.float32
bf16 = jnp.bfloat16
f16 = jnp.float16
MM = dict(preferred_element_type=f32)


def up(value, unit):
    return -(-value // unit) * unit


def params(megabytes=20):
    return pltpu.CompilerParams(vmem_limit_bytes=megabytes * 1024 * 1024)


def split(value, parts):
    pieces = []
    for _ in range(parts - 1):
        high = value.astype(bf16)
        pieces.append(high)
        value = value - high.astype(f32)
    pieces.append(value.astype(bf16))
    return pieces


def matmul(a, b):
    return lax.dot_general(a, b, (((1,), (0,)), ((), ())), **MM)


def matmul_nt(a, b):
    return lax.dot_general(a, b, (((1,), (1,)), ((), ())), **MM)


def one_hot(frames, index_row):
    rows = lax.broadcasted_iota(jnp.int32, (frames, index_row.shape[1]), 0)
    return jnp.where(rows == index_row, 1.0, 0.0).astype(bf16)


def turn(row):
    square = jnp.broadcast_to(row.astype(f32), (LANES, row.shape[1]))
    return jnp.transpose(square)[:, 0:1].astype(jnp.int32)


def padded(value, rows):
    return jnp.pad(value, ((0, rows - value.shape[0]), (0, 0)))


vmem = pl.BlockSpec(memory_space=VMEM)
smem = pl.BlockSpec(memory_space=SMEM)


def pick_residual(index, residual_t):
    outputs, frames = residual_t.shape
    rows = up(outputs, 16)
    steps, picks = index.shape

    def body(index_ref, residual_ref, *out_ref):
        both = jnp.concatenate(split(padded(residual_ref[...], rows), 2), 0)
        for step in range(steps):
            found = matmul(both, one_hot(frames, index_ref[step : step + 1, :]))
            out_ref[step][...] = found[:rows] + found[rows:]

    return pl.pallas_call(
        body,
        in_specs=[vmem, vmem],
        out_specs=(vmem,) * steps,
        out_shape=(jax.ShapeDtypeStruct((rows, picks), f32),) * steps,
        compiler_params=params(),
        name="pick_residual",
    )(index, residual_t)


def norm_rows(squares, kinds):
    width = squares.shape[1]
    norm = split(-0.5 * squares, 3)
    ones = jnp.ones((3, width), bf16)
    zeros = jnp.zeros((6, width), bf16)
    norm = jnp.concatenate(norm, 0)
    pieces = []
    for kind in kinds:
        if kind == 0:
            pieces.append(zeros)
        elif kind == 1:
            pieces.append(jnp.concatenate([norm, ones], 0))
        else:
            pieces.append(jnp.concatenate([ones, norm], 0))
    return jnp.concatenate(pieces, 0)


def pick_features(owners, index, features_t, rules):
    width, frames = features_t.shape
    depth = up(width + 18, 16)
    steps, picks = index.shape
    kinds = ((2, 0, 1), (0, 2, 2))

    def body(owners_ref, index_ref, features_ref, *out_ref):
        features = features_ref[...]
        rest = jnp.zeros((depth - width - 18, picks), bf16)
        for step in range(steps):
            picked = matmul(features, one_hot(frames, index_ref[step : step + 1, :]))
            squares = jnp.sum(picked * picked, axis=0, keepdims=True)
            out_ref[step][0:width, :] = picked.astype(bf16)
            out_ref[step][width:depth, :] = jnp.concatenate([norm_rows(squares, kinds[step]), rest], 0)
        row = lax.axis_index("rows")
        for (step, rule), take_ref in zip(rules, out_ref[steps:]):
            take = jnp.where(rule(row, owners_ref[step]), 1.0, 0.0)
            take_ref[...] = jnp.full(take_ref.shape, take, f32)

    return pl.pallas_call(
        body,
        in_specs=[smem, vmem, vmem],
        out_specs=(vmem,) * (steps + len(rules)),
        out_shape=(jax.ShapeDtypeStruct((depth, picks), bf16),) * steps
        + (jax.ShapeDtypeStruct((1, picks), f32),) * len(rules),
        compiler_params=params(),
        name="pick_features",
    )(owners, index, features_t)


def lane_start(value, unit):
    return pl.ds(pl.multiple_of(value * unit, unit), unit)


def piece_col(piece):
    mine = lax.axis_index("cols")
    return ((mine // 2) ^ (piece // 2)) * 2 + ((mine % 2) ^ (piece % 2))


def fold(update):
    half = update.shape[0] // 2
    return jnp.concatenate([update[:half], update[half:]], 1).astype(bf16)


def prepare(features_t, inverse, picks):
    width, frames = features_t.shape
    depth = up(width + 18, 16)
    steps, mine, block = inverse.shape

    def body(features_ref, inverse_ref, local_ref, *stacked_ref):
        features = features_ref[...]
        wide = features.astype(f32)
        squares = jnp.sum(wide * wide, axis=0, keepdims=True)
        local_ref[0:width, :] = features
        rest = jnp.zeros((depth - width - 18, frames), bf16)
        local_ref[width:depth, :] = jnp.concatenate([norm_rows(squares, (1, 1, 0)), rest], 0)
        for step in range(steps):
            for k in range(block // picks):
                high, low = split(inverse_ref[step, :, lane_start(piece_col(k), picks)], 2)
                stacked_ref[step][:, k * picks : (k + 1) * picks] = jnp.concatenate([high, low], 0)

    return pl.pallas_call(
        body,
        in_specs=[vmem, vmem],
        out_specs=(vmem,) * (1 + steps),
        out_shape=(jax.ShapeDtypeStruct((depth, frames), bf16),)
        + (jax.ShapeDtypeStruct((2 * mine, block), bf16),) * steps,
        compiler_params=params(),
        name="prepare",
    )(features_t, inverse)


def block_update(picked, stacked, scaled):
    rows, _ = picked.shape
    mine = stacked.shape[0] // 2

    def body(stacked_ref, picked_ref, out_ref):
        product = matmul_nt(jnp.concatenate(split(picked_ref[...], 2), 0), stacked_ref[...])
        product = product[:rows] + product[rows:]
        out_ref[...] = fold((product[:, :mine] + product[:, mine:]) * scaled)

    return pl.pallas_call(
        body,
        in_specs=[vmem, vmem],
        out_specs=vmem,
        out_shape=jax.ShapeDtypeStruct((rows // 2, 2 * mine), bf16),
        compiler_params=params(),
    )(stacked, picked)


def meeting_kernel(owners, index, pieces, second, scale):
    depth, picks = second.shape
    count = len(pieces)

    def body(owners_ref, index_ref, second_ref, *refs):
        pieces_ref, out_ref = refs[:count], refs[-1]
        for k in range(count):
            inner = matmul(jnp.transpose(pieces_ref[k][...]), second_ref[...])
            kernel = jnp.exp2(inner * scale).astype(bf16)
            if k == 0:
                same = turn(index_ref[0:1, :]) == index_ref[1:2, :]
                bonus = jnp.where(owners_ref[0] == owners_ref[1], penalty, 0.0)
                kernel = kernel + jnp.where(same, bonus, 0.0).astype(bf16)
            out_ref[k * picks : (k + 1) * picks, :] = kernel

    return pl.pallas_call(
        body,
        in_specs=[smem, vmem, vmem] + [vmem] * count,
        out_specs=vmem,
        out_shape=jax.ShapeDtypeStruct((count * picks, picks), bf16),
        cost_estimate=pl.CostEstimate(
            flops=2 * count * picks * picks * depth, transcendentals=count * picks * picks, bytes_accessed=10**6
        ),
        compiler_params=params(),
        name="meeting_kernel",
    )(owners, index, second, *pieces)


def advance(kernel, before, pieces, scaled):
    rows, picks = before.shape
    block = kernel.shape[0]
    count = len(pieces)

    def body(kernel_ref, before_ref, *refs):
        pieces_ref, out_ref, canon = refs[:count], refs[-2], refs[-1]
        unfold(pieces_ref, pieces[0].shape[0] * 2 // rows, picks, canon)
        out_ref[...] = (before_ref[...] - matmul(canon[...], kernel_ref[...])) * scaled

    return pl.pallas_call(
        body,
        in_specs=[vmem] * (2 + count),
        out_specs=vmem,
        out_shape=jax.ShapeDtypeStruct((rows, picks), f32),
        scratch_shapes=[pltpu.VMEM((rows, block), bf16)],
        compiler_params=params(),
        name="advance",
    )(kernel, before, *pieces)


def block_kernel(pieces, local, scale):
    depth, frames = local.shape
    picks = pieces[0].shape[1]
    count = len(pieces)
    block = picks * count
    tile = min(512, frames)

    def body(local_ref, *refs):
        pieces_ref, out_ref = refs[:count], refs[-1]
        for k in range(count):
            turned = jnp.transpose(pieces_ref[k][...])
            for start in range(0, frames, tile):
                inner = matmul(turned, local_ref[:, start : start + tile])
                out_ref[k * picks : (k + 1) * picks, start : start + tile] = jnp.exp2(inner * scale).astype(bf16)

    return pl.pallas_call(
        body,
        in_specs=[vmem] * (1 + count),
        out_specs=vmem,
        out_shape=jax.ShapeDtypeStruct((block, frames), bf16),
        cost_estimate=pl.CostEstimate(
            flops=2 * block * frames * depth, transcendentals=block * frames, bytes_accessed=10**7
        ),
        compiler_params=params(),
    )(local, *pieces)


def unfold(pieces_ref, parts, picks, canon):
    half, width = pieces_ref[0].shape[0] // parts, pieces_ref[0].shape[1]
    mine = width // 2
    count = len(pieces_ref)
    lanes = lax.broadcasted_iota(jnp.int32, (half, width), 1)
    low = lanes < mine
    row, col = lax.axis_index("rows"), lax.axis_index("cols")
    core = col % 2
    for k in range(0, count, 2):
        for r in range(parts):
            here = pieces_ref[k][r * half : (r + 1) * half, :].astype(f32)
            other = pieces_ref[k + 1][r * half : (r + 1) * half, :].astype(f32)
            a = jnp.where(core == 0, here, other)
            b = jnp.where(core == 0, other, here)
            upper = jnp.where(low, a, pltpu.roll(b, mine, 1))
            lower = jnp.where(low, pltpu.roll(a, mine, 1), b)
            pair = (row ^ r) * (count // 2) + ((col // 2) ^ (k // 2))
            from_col = pair * width // picks
            place = ((from_col // 2) ^ (col // 2)) * 2 + ((from_col % 2) ^ core)
            place = pl.ds(pl.multiple_of(place * picks + pair * width % picks, width), width)
            canon[0:half, place] = upper.astype(bf16)
            canon[half:, place] = lower.astype(bf16)


def apply_update(owners, pieces, kernel, index, step, residual_t, coeffs_t):
    outputs, frames = residual_t.shape
    block = kernel.shape[0]
    picks = index.shape[1]
    count = len(pieces)
    rows = up(outputs, 16)
    tile = min(1024, frames)

    def body(owners_ref, index_ref, kernel_ref, residual_ref, coeffs_ref, *refs):
        pieces_ref = refs[:count]
        new_residual_ref, new_coeffs_ref, canon, own, places = refs[count:]
        here = pl.program_id(0)

        @pl.when(here == 0)
        def _():
            unfold(pieces_ref, pieces[0].shape[0] * 2 // rows, picks, canon)
            mine = canon[:, 0:picks]
            own[...] = jnp.where(lax.axis_index("rows") == owners_ref[step], mine, jnp.zeros_like(mine))
            places[...] = turn(index_ref[step : step + 1, :])

        change = matmul(canon[...], kernel_ref[:, lane_start(here, tile)])
        frame = lax.broadcasted_iota(jnp.int32, (picks, tile), 1) + here * tile
        hot = jnp.where(frame == places[...], 1.0, 0.0).astype(bf16)
        put = matmul(own[...], hot)
        new_residual_ref[...] = residual_ref[...] - (change + penalty * put)[:outputs]
        new_coeffs_ref[...] = coeffs_ref[...] + put[:outputs]

    strip = pl.BlockSpec((outputs, tile), lambda i: (0, i))
    return pl.pallas_call(
        body,
        grid=(frames // tile,),
        in_specs=[smem, vmem, vmem, strip, strip] + [vmem] * count,
        out_specs=(strip, strip),
        out_shape=(
            jax.ShapeDtypeStruct((outputs, frames), f32),
            jax.ShapeDtypeStruct((outputs, frames), f32),
        ),
        scratch_shapes=[
            pltpu.VMEM((rows, block), bf16),
            pltpu.VMEM((rows, picks), bf16),
            pltpu.VMEM((picks, 1), jnp.int32),
        ],
        cost_estimate=pl.CostEstimate(
            flops=2 * rows * block * frames, transcendentals=0, bytes_accessed=2 * block * frames
        ),
        compiler_params=params(),
    )(owners, index, kernel, residual_t, coeffs_t, *pieces)


class Sender:
    def __init__(self, rows, cols):
        self.rows, self.cols, self.chips = rows, cols, cols // 2

    def send(self, value, row=None, chip_step=0, core_step=0):
        pairs = []
        for i in range(self.rows * self.cols):
            at, col = i // self.cols, i % self.cols
            to = at if row is None else row(at)
            if to is None:
                continue
            col = ((col // 2) ^ chip_step) * 2 + ((col % 2) ^ core_step)
            pairs.append((i, to * self.cols + col))
        return lax.ppermute(value, ("rows", "cols"), pairs)

    def spread(self, value, moves, takes):
        for move, take in zip(moves, takes):
            other = self.send(value, row=move)
            value = jnp.where(take > 0.5, other, value)
        return value

    def over_rows(self, value):
        steps = range(1, self.rows)
        got = {k: self.send(value, row=lambda at, k=k: at ^ k) for k in steps}
        return [value] + [got[k] for k in range(1, self.rows)]

    def over_cores(self, values):
        return [side for v in values for side in (v, self.send(v, core_step=1))]

    def over_cols(self, value):
        values = [value] + [self.send(value, chip_step=k) for k in range(1, self.chips)]
        return self.over_cores(values)


def doubling(rows):
    steps = [1 << k for k in range(rows.bit_length() - 1)]
    moves = [lambda at, step=step: at ^ step for step in steps]
    rules = [lambda row, owner, step=step: ((row ^ owner) & step) != 0 for step in steps]
    return moves, rules


def per_device_pieces(rows, cols, features, residual, coeffs, block_inverse, block_index, owners):
    scale = 2.0 / features.shape[1] * 1.4426950408889634
    sender = Sender(rows, cols)
    picks = block_index.shape[1]
    moves, rules = doubling(rows)
    block = block_inverse.shape[2]
    bound = 6.0 + (block + penalty) * block * 6.0 * 0.0234375
    scaled = 2.0 ** -max(0, math.ceil(math.log2(bound / 60000.0)))
    features_t, residual_t, coeffs_t = features.T, residual.T, coeffs.T
    first, second = pick_residual(block_index, residual_t)
    first_block, second_block, *takes = pick_features(
        owners, block_index, features_t, [(step, rule) for step in range(2) for rule in rules]
    )
    local, *stacked = prepare(features_t, block_inverse, picks)
    first = sender.over_cols(sender.spread(first.astype(f16), moves, takes))
    first_block = sender.over_cols(sender.spread(first_block, moves, takes))
    second = sender.spread(second.astype(f16), moves, takes[len(rules) :]).astype(f32)
    second_block = sender.spread(second_block, moves, takes[len(rules) :])
    update = block_update(jnp.concatenate(first, 1).astype(f32), stacked[0], 1.0)
    update = sender.over_cols(jnp.concatenate(sender.over_rows(update), 0))
    meeting = meeting_kernel(owners, block_index, first_block, second_block, scale)
    second = sender.over_cols(advance(meeting, second, update, scaled).astype(f16))
    first_kernel = block_kernel(first_block, local, scale)
    later = block_update(jnp.concatenate(second, 1).astype(f32), stacked[1], 1.0 / scaled)
    later = sender.over_cols(jnp.concatenate(sender.over_rows(later), 0))
    second_block = sender.over_cols(second_block)
    second_kernel = block_kernel(second_block, local, scale)
    residual_t, coeffs_t = apply_update(
        owners, update, first_kernel, block_index, 0, residual_t, coeffs_t
    )
    residual_t, coeffs_t = apply_update(
        owners, later, second_kernel, block_index, 1, residual_t, coeffs_t
    )
    return (coeffs_t.T, residual_t.T)


def from_root(value, axis, source):
    kept = jnp.where(lax.axis_index(axis) == source, value, 0).astype(value.dtype)
    return lax.psum(kept, axis)


def per_device_plain(features, residual, coeffs, block_inverse, block_index, owners):
    frame_count = features.shape[0]
    feature_width = features.shape[1]
    per_col = block_index.shape[1]
    row_block = min(512, frame_count)
    exponent = -1.0 / feature_width
    my_row = lax.axis_index("rows")
    my_col = lax.axis_index("cols")
    squares = jnp.sum(jnp.square(features.astype(jnp.float32)), axis=1)
    feature_blocks = features.reshape(frame_count // row_block, row_block, feature_width)
    norm_blocks = squares.reshape(frame_count // row_block, row_block)
    for step_id in range(block_index.shape[0]):
        chosen_rows = block_index[step_id]
        owner_row = owners[step_id]
        mine_feat = jnp.take(features, chosen_rows, axis=0)
        mine_res = jnp.take(residual, chosen_rows, axis=0)
        row_piece = from_root(mine_feat, "rows", owner_row)
        chosen = lax.all_gather(row_piece, "cols", axis=0, tiled=True)
        res_piece = from_root(mine_res, "rows", owner_row)
        picked_res = lax.all_gather(res_piece, "cols", axis=0, tiled=True)
        my_update = jnp.dot(
            block_inverse[step_id],
            picked_res,
            precision=lax.Precision.HIGHEST,
            preferred_element_type=jnp.float32,
        ).astype(jnp.bfloat16)
        update = lax.all_gather(my_update, ("rows", "cols"), axis=0, tiled=True)
        chosen_norms = jnp.sum(jnp.square(chosen.astype(jnp.float32)), axis=1)

        def kernel_rows(operands):
            block_rows, block_norms = operands
            inner = lax.dot_general(
                block_rows, chosen, (((1,), (1,)), ((), ())), preferred_element_type=jnp.float32
            )
            distance = block_norms[:, None] + chosen_norms[None, :] - 2.0 * inner
            kernel = jnp.exp(distance * exponent).astype(jnp.bfloat16)
            return jnp.dot(kernel, update, preferred_element_type=jnp.float32)

        change = lax.map(kernel_rows, (feature_blocks, norm_blocks)).reshape(frame_count, -1)
        residual = residual - change
        is_owner = jnp.where(my_row == owner_row, 1.0, 0.0).astype(jnp.float32)
        mine_update = (
            lax.dynamic_slice_in_dim(update, my_col * per_col, per_col, 0).astype(jnp.float32)
            * is_owner
        )
        residual = residual.at[chosen_rows].add(-penalty * mine_update)
        coeffs = coeffs.at[chosen_rows].add(mine_update)
    return (coeffs, residual)


def power_of_two(value):
    return value & (value - 1) == 0


def solution(mesh):
    rows, cols = mesh.shape["rows"], mesh.shape["cols"]
    in_specs = (
        P(("rows", "cols"), None),
        P(("rows", "cols"), None),
        P(("rows", "cols"), None),
        P(None, ("rows", "cols"), None),
        P(None, "cols"),
        P(),
    )
    out_specs = (P(("rows", "cols"), None), P(("rows", "cols"), None))

    def per_device(features, residual, coeffs, block_inverse, block_index, owners):
        args = (features, residual, coeffs, block_inverse, block_index, owners)
        return per_device_pieces(rows, cols, *args) if fits(*args) else per_device_plain(*args)

    def fits(features, residual, coeffs, block_inverse, block_index, owners):
        return (
            small
            and block_index.shape[0] == 2
            and block_index.shape[1] % LANES == 0
            and 2 * block_inverse.shape[1] == LANES
            and features.shape[0] % 1024 == 0
        )

    small = power_of_two(rows) and power_of_two(cols) and 2 <= rows <= 8 and 4 <= cols <= 16
    return jax.shard_map(
        per_device, mesh=mesh, in_specs=in_specs, out_specs=out_specs, check_vma=False
    )
```

```python
import math

import jax
import jax.numpy as jnp
from jax import lax
from jax.experimental import pallas as pl
from jax.experimental.pallas import tpu as pltpu
from jax.sharding import PartitionSpec as P


penalty = 0.5
LANES = 128
VMEM = pltpu.MemorySpace.VMEM
SMEM = pltpu.MemorySpace.SMEM
f32 = jnp.float32
bf16 = jnp.bfloat16
f16 = jnp.float16
MM = dict(preferred_element_type=f32)


def up(value, unit):
    return -(-value // unit) * unit


def params(megabytes=20):
    return pltpu.CompilerParams(vmem_limit_bytes=megabytes * 1024 * 1024)


def split(value, parts):
    pieces = []
    for _ in range(parts - 1):
        high = value.astype(bf16)
        pieces.append(high)
        value = value - high.astype(f32)
    pieces.append(value.astype(bf16))
    return pieces


def matmul(a, b):
    return lax.dot_general(a, b, (((1,), (0,)), ((), ())), **MM)


def matmul_nt(a, b):
    return lax.dot_general(a, b, (((1,), (1,)), ((), ())), **MM)


def one_hot(frames, index_row):
    rows = lax.broadcasted_iota(jnp.int32, (frames, index_row.shape[1]), 0)
    return jnp.where(rows == index_row, 1.0, 0.0).astype(bf16)


def turn(row):
    square = jnp.broadcast_to(row.astype(f32), (LANES, row.shape[1]))
    return jnp.transpose(square)[:, 0:1].astype(jnp.int32)


def padded(value, rows):
    return jnp.pad(value, ((0, rows - value.shape[0]), (0, 0)))


vmem = pl.BlockSpec(memory_space=VMEM)
smem = pl.BlockSpec(memory_space=SMEM)


def pick_residual(index, residual_t):
    outputs, frames = residual_t.shape
    rows = up(outputs, 16)
    steps, picks = index.shape

    def body(index_hbm, residual_hbm, *refs):
        out_ref, (index_ref, residual_ref, index_sem, residual_sem) = refs[:steps], refs[steps:]
        index_copy = pltpu.make_async_copy(index_hbm, index_ref, index_sem)
        residual_copy = pltpu.make_async_copy(residual_hbm, residual_ref, residual_sem)
        residual_copy.start()
        index_copy.start()
        index_copy.wait()
        residual_copy.wait()
        both = jnp.concatenate(split(padded(residual_ref[...], rows), 2), 0)
        for step in range(steps):
            found = matmul(both, one_hot(frames, index_ref[step : step + 1, :]))
            out_ref[step][...] = found[:rows] + found[rows:]

    return pl.pallas_call(
        body,
        in_specs=[pl.BlockSpec(memory_space=pl.ANY)] * 2,
        out_specs=(vmem,) * steps,
        out_shape=(jax.ShapeDtypeStruct((rows, picks), f32),) * steps,
        scratch_shapes=[
            pltpu.VMEM((steps, picks), jnp.int32),
            pltpu.VMEM((outputs, frames), f32),
            pltpu.SemaphoreType.DMA,
            pltpu.SemaphoreType.DMA,
        ],
        compiler_params=params(),
        name="pick_residual",
    )(index, residual_t)


def norm_rows(squares, kinds):
    width = squares.shape[1]
    norm = split(-0.5 * squares, 3)
    ones = jnp.ones((3, width), bf16)
    zeros = jnp.zeros((6, width), bf16)
    norm = jnp.concatenate(norm, 0)
    pieces = []
    for kind in kinds:
        if kind == 0:
            pieces.append(zeros)
        elif kind == 1:
            pieces.append(jnp.concatenate([norm, ones], 0))
        else:
            pieces.append(jnp.concatenate([ones, norm], 0))
    return jnp.concatenate(pieces, 0)


def pick_features(owners, index, features_t, rules):
    width, frames = features_t.shape
    depth = up(width + 18, 16)
    steps, picks = index.shape
    kinds = ((2, 0, 1), (0, 2, 2))

    def body(owners_ref, index_ref, features_ref, *out_ref):
        features = features_ref[...]
        rest = jnp.zeros((depth - width - 18, picks), bf16)
        for step in range(steps):
            picked = matmul(features, one_hot(frames, index_ref[step : step + 1, :]))
            squares = jnp.sum(picked * picked, axis=0, keepdims=True)
            out_ref[step][0:width, :] = picked.astype(bf16)
            out_ref[step][width:depth, :] = jnp.concatenate([norm_rows(squares, kinds[step]), rest], 0)
        row = lax.axis_index("rows")
        for (step, rule), take_ref in zip(rules, out_ref[steps:]):
            take = jnp.where(rule(row, owners_ref[step]), 1.0, 0.0)
            take_ref[...] = jnp.full(take_ref.shape, take, f32)

    return pl.pallas_call(
        body,
        in_specs=[smem, vmem, vmem],
        out_specs=(vmem,) * (steps + len(rules)),
        out_shape=(jax.ShapeDtypeStruct((depth, picks), bf16),) * steps
        + (jax.ShapeDtypeStruct((1, picks), f32),) * len(rules),
        compiler_params=params(),
        name="pick_features",
    )(owners, index, features_t)


def lane_start(value, unit):
    return pl.ds(pl.multiple_of(value * unit, unit), unit)


def piece_col(piece):
    mine = lax.axis_index("cols")
    return ((mine // 2) ^ (piece // 2)) * 2 + ((mine % 2) ^ (piece % 2))


def fold(update):
    half = update.shape[0] // 2
    return jnp.concatenate([update[:half], update[half:]], 1).astype(bf16)


def localize(features_t):
    width, frames = features_t.shape
    depth = up(width + 18, 16)

    def body(features_ref, local_ref):
        features = features_ref[...]
        wide = features.astype(f32)
        squares = jnp.sum(wide * wide, axis=0, keepdims=True)
        local_ref[0:width, :] = features
        rest = jnp.zeros((depth - width - 18, frames), bf16)
        local_ref[width:depth, :] = jnp.concatenate([norm_rows(squares, (1, 1, 0)), rest], 0)

    return pl.pallas_call(
        body,
        in_specs=[vmem],
        out_specs=vmem,
        out_shape=jax.ShapeDtypeStruct((depth, frames), bf16),
        compiler_params=params(),
        name="localize",
    )(features_t)


def prepare(inverse, picks):
    steps, mine, block = inverse.shape

    def body(inverse_ref, *stacked_ref):
        for step in range(steps):
            for k in range(block // picks):
                high, low = split(inverse_ref[step, :, lane_start(piece_col(k), picks)], 2)
                stacked_ref[step][:, k * picks : (k + 1) * picks] = jnp.concatenate([high, low], 0)

    return pl.pallas_call(
        body,
        in_specs=[vmem],
        out_specs=(vmem,) * steps,
        out_shape=(jax.ShapeDtypeStruct((2 * mine, block), bf16),) * steps,
        compiler_params=params(),
        name="prepare",
    )(inverse)


def block_update(picked, stacked, scaled):
    rows, _ = picked.shape
    mine = stacked.shape[0] // 2

    def body(stacked_ref, picked_ref, out_ref):
        product = matmul_nt(jnp.concatenate(split(picked_ref[...], 2), 0), stacked_ref[...])
        product = product[:rows] + product[rows:]
        out_ref[...] = fold((product[:, :mine] + product[:, mine:]) * scaled)

    return pl.pallas_call(
        body,
        in_specs=[vmem, vmem],
        out_specs=vmem,
        out_shape=jax.ShapeDtypeStruct((rows // 2, 2 * mine), bf16),
        compiler_params=params(),
    )(stacked, picked)


def meeting_kernel(owners, index, pieces, second, scale):
    depth, picks = second.shape
    count = len(pieces)

    def body(owners_ref, index_ref, second_ref, *refs):
        pieces_ref, out_ref = refs[:count], refs[-1]
        for k in range(count):
            inner = matmul(jnp.transpose(pieces_ref[k][...]), second_ref[...])
            kernel = jnp.exp2(inner * scale).astype(bf16)
            if k == 0:
                same = turn(index_ref[0:1, :]) == index_ref[1:2, :]
                bonus = jnp.where(owners_ref[0] == owners_ref[1], penalty, 0.0)
                kernel = kernel + jnp.where(same, bonus, 0.0).astype(bf16)
            out_ref[k * picks : (k + 1) * picks, :] = kernel

    return pl.pallas_call(
        body,
        in_specs=[smem, vmem, vmem] + [vmem] * count,
        out_specs=vmem,
        out_shape=jax.ShapeDtypeStruct((count * picks, picks), bf16),
        cost_estimate=pl.CostEstimate(
            flops=2 * count * picks * picks * depth, transcendentals=count * picks * picks, bytes_accessed=10**6
        ),
        compiler_params=params(),
        name="meeting_kernel",
    )(owners, index, second, *pieces)


def advance(kernel, before, pieces, scaled):
    rows, picks = before.shape
    block = kernel.shape[0]
    count = len(pieces)

    def body(kernel_ref, before_ref, *refs):
        pieces_ref, out_ref, canon = refs[:count], refs[-2], refs[-1]
        unfold(pieces_ref, pieces[0].shape[0] * 2 // rows, picks, canon)
        out_ref[...] = (before_ref[...] - matmul(canon[...], kernel_ref[...])) * scaled

    return pl.pallas_call(
        body,
        in_specs=[vmem] * (2 + count),
        out_specs=vmem,
        out_shape=jax.ShapeDtypeStruct((rows, picks), f32),
        scratch_shapes=[pltpu.VMEM((rows, block), bf16)],
        compiler_params=params(),
        name="advance",
    )(kernel, before, *pieces)


def block_kernel(pieces, local, scale):
    depth, frames = local.shape
    picks = pieces[0].shape[1]
    count = len(pieces)
    block = picks * count
    tile = min(512, frames)

    def body(local_ref, *refs):
        pieces_ref, out_ref = refs[:count], refs[-1]
        for k in range(count):
            turned = jnp.transpose(pieces_ref[k][...])
            for start in range(0, frames, tile):
                inner = matmul(turned, local_ref[:, start : start + tile])
                out_ref[k * picks : (k + 1) * picks, start : start + tile] = jnp.exp2(inner * scale).astype(bf16)

    return pl.pallas_call(
        body,
        in_specs=[vmem] * (1 + count),
        out_specs=vmem,
        out_shape=jax.ShapeDtypeStruct((block, frames), bf16),
        cost_estimate=pl.CostEstimate(
            flops=2 * block * frames * depth, transcendentals=block * frames, bytes_accessed=10**7
        ),
        compiler_params=params(),
    )(local, *pieces)


def unfold(pieces_ref, parts, picks, canon):
    half, width = pieces_ref[0].shape[0] // parts, pieces_ref[0].shape[1]
    mine = width // 2
    count = len(pieces_ref)
    lanes = lax.broadcasted_iota(jnp.int32, (half, width), 1)
    low = lanes < mine
    row, col = lax.axis_index("rows"), lax.axis_index("cols")
    core = col % 2
    for k in range(0, count, 2):
        for r in range(parts):
            here = pieces_ref[k][r * half : (r + 1) * half, :].astype(f32)
            other = pieces_ref[k + 1][r * half : (r + 1) * half, :].astype(f32)
            a = jnp.where(core == 0, here, other)
            b = jnp.where(core == 0, other, here)
            upper = jnp.where(low, a, pltpu.roll(b, mine, 1))
            lower = jnp.where(low, pltpu.roll(a, mine, 1), b)
            pair = (row ^ r) * (count // 2) + ((col // 2) ^ (k // 2))
            from_col = pair * width // picks
            place = ((from_col // 2) ^ (col // 2)) * 2 + ((from_col % 2) ^ core)
            place = pl.ds(pl.multiple_of(place * picks + pair * width % picks, width), width)
            canon[0:half, place] = upper.astype(bf16)
            canon[half:, place] = lower.astype(bf16)


def apply_update(owners, pieces, kernels, index, step, residual_t, coeffs_t):
    outputs, frames = residual_t.shape
    block = sum(kernel.shape[0] for kernel in kernels)
    picks = index.shape[1]
    count = len(pieces)
    rows = up(outputs, 16)
    tile = min(1024, frames)

    def body(owners_ref, index_ref, residual_ref, coeffs_ref, *refs):
        kernels_ref, refs = refs[: len(kernels)], refs[len(kernels) :]
        pieces_ref = refs[:count]
        new_residual_ref, new_coeffs_ref, canon, own, places = refs[count:]
        here = pl.program_id(0)

        @pl.when(here == 0)
        def _():
            unfold(pieces_ref, pieces[0].shape[0] * 2 // rows, picks, canon)
            mine = canon[:, 0:picks]
            own[...] = jnp.where(lax.axis_index("rows") == owners_ref[step], mine, jnp.zeros_like(mine))
            places[...] = turn(index_ref[step : step + 1, :])

        change, first = 0.0, 0
        for kernel_ref in kernels_ref:
            last = first + kernel_ref.shape[0]
            change = change + matmul(canon[:, first:last], kernel_ref[:, lane_start(here, tile)])
            first = last
        frame = lax.broadcasted_iota(jnp.int32, (picks, tile), 1) + here * tile
        hot = jnp.where(frame == places[...], 1.0, 0.0).astype(bf16)
        put = matmul(own[...], hot)
        new_residual_ref[...] = residual_ref[:, lane_start(here, tile)] - (change + penalty * put)[:outputs]
        new_coeffs_ref[...] = coeffs_ref[:, lane_start(here, tile)] + put[:outputs]

    strip = pl.BlockSpec((outputs, tile), lambda i: (0, i))
    return pl.pallas_call(
        body,
        grid=(frames // tile,),
        in_specs=[smem, vmem, vmem, vmem] + [vmem] * (len(kernels) + count),
        out_specs=(strip, strip),
        out_shape=(
            jax.ShapeDtypeStruct((outputs, frames), f32),
            jax.ShapeDtypeStruct((outputs, frames), f32),
        ),
        scratch_shapes=[
            pltpu.VMEM((rows, block), bf16),
            pltpu.VMEM((rows, picks), bf16),
            pltpu.VMEM((picks, 1), jnp.int32),
        ],
        cost_estimate=pl.CostEstimate(
            flops=2 * rows * block * frames, transcendentals=0, bytes_accessed=2 * block * frames
        ),
        compiler_params=params(),
    )(owners, index, residual_t, coeffs_t, *kernels, *pieces)


class Sender:
    def __init__(self, rows, cols):
        self.rows, self.cols, self.chips = rows, cols, cols // 2

    def send(self, value, row=None, chip_step=0, core_step=0):
        pairs = []
        for i in range(self.rows * self.cols):
            at, col = i // self.cols, i % self.cols
            to = at if row is None else row(at)
            if to is None:
                continue
            col = ((col // 2) ^ chip_step) * 2 + ((col % 2) ^ core_step)
            pairs.append((i, to * self.cols + col))
        return lax.ppermute(value, ("rows", "cols"), pairs)

    def spread(self, value, moves, takes):
        for move, take in zip(moves, takes):
            other = self.send(value, row=move)
            value = jnp.where(take > 0.5, other, value)
        return value

    def over_rows(self, value):
        steps = range(1, self.rows)
        got = {k: self.send(value, row=lambda at, k=k: at ^ k) for k in steps}
        return [value] + [got[k] for k in range(1, self.rows)]

    def over_cores(self, values):
        return [side for v in values for side in (v, self.send(v, core_step=1))]

    def over_cols(self, value):
        values = [value] + [self.send(value, chip_step=k) for k in range(1, self.chips)]
        return self.over_cores(values)


def doubling(rows):
    steps = [1 << k for k in range(rows.bit_length() - 1)]
    moves = [lambda at, step=step: at ^ step for step in steps]
    rules = [lambda row, owner, step=step: ((row ^ owner) & step) != 0 for step in steps]
    return moves, rules


def per_device_pieces(rows, cols, features, residual, coeffs, block_inverse, block_index, owners):
    scale = 2.0 / features.shape[1] * 1.4426950408889634
    sender = Sender(rows, cols)
    picks = block_index.shape[1]
    moves, rules = doubling(rows)
    block = block_inverse.shape[2]
    bound = 6.0 + (block + penalty) * block * 6.0 * 0.0234375
    scaled = 2.0 ** -max(0, math.ceil(math.log2(bound / 60000.0)))
    features_t, residual_t, coeffs_t = features.T, residual.T, coeffs.T
    first, second = pick_residual(block_index, residual_t)
    first_block, second_block, *takes = pick_features(
        owners, block_index, features_t, [(step, rule) for step in range(2) for rule in rules]
    )
    stacked = prepare(block_inverse, picks)
    local = localize(features_t)
    first = sender.over_cols(sender.spread(first.astype(f16), moves, takes))
    first_block = sender.over_cols(sender.spread(first_block, moves, takes))
    depth = second_block.shape[0]
    both = jnp.concatenate([second_block.astype(f16), second.astype(f16)], 0)
    both = sender.spread(both, moves, takes[len(rules) :])
    second_block, second = both[:depth].astype(bf16), both[depth:].astype(f32)
    update = block_update(jnp.concatenate(first, 1).astype(f32), stacked[0], 1.0)
    update = sender.over_cols(jnp.concatenate(sender.over_rows(update), 0))
    meeting = meeting_kernel(owners, block_index, first_block, second_block, scale)
    second = sender.over_cols(advance(meeting, second, update, scaled).astype(f16))
    near = len(first_block) // 2
    near_kernel = block_kernel(first_block[:near], local, scale)
    far_kernel = block_kernel(first_block[near:], local, scale)
    later = block_update(jnp.concatenate(second, 1).astype(f32), stacked[1], 1.0 / scaled)
    later = sender.over_cols(jnp.concatenate(sender.over_rows(later), 0))
    second_block = sender.over_cols(second_block)
    second_kernel = block_kernel(second_block, local, scale)
    residual_t, coeffs_t = apply_update(
        owners, update, (near_kernel, far_kernel), block_index, 0, residual_t, coeffs_t
    )
    residual_t, coeffs_t = apply_update(
        owners, later, (second_kernel,), block_index, 1, residual_t, coeffs_t
    )
    return (coeffs_t.T, residual_t.T)


def from_root(value, axis, source):
    kept = jnp.where(lax.axis_index(axis) == source, value, 0).astype(value.dtype)
    return lax.psum(kept, axis)


def per_device_plain(features, residual, coeffs, block_inverse, block_index, owners):
    frame_count = features.shape[0]
    feature_width = features.shape[1]
    per_col = block_index.shape[1]
    row_block = min(512, frame_count)
    exponent = -1.0 / feature_width
    my_row = lax.axis_index("rows")
    my_col = lax.axis_index("cols")
    squares = jnp.sum(jnp.square(features.astype(jnp.float32)), axis=1)
    feature_blocks = features.reshape(frame_count // row_block, row_block, feature_width)
    norm_blocks = squares.reshape(frame_count // row_block, row_block)
    for step_id in range(block_index.shape[0]):
        chosen_rows = block_index[step_id]
        owner_row = owners[step_id]
        mine_feat = jnp.take(features, chosen_rows, axis=0)
        mine_res = jnp.take(residual, chosen_rows, axis=0)
        row_piece = from_root(mine_feat, "rows", owner_row)
        chosen = lax.all_gather(row_piece, "cols", axis=0, tiled=True)
        res_piece = from_root(mine_res, "rows", owner_row)
        picked_res = lax.all_gather(res_piece, "cols", axis=0, tiled=True)
        my_update = jnp.dot(
            block_inverse[step_id],
            picked_res,
            precision=lax.Precision.HIGHEST,
            preferred_element_type=jnp.float32,
        ).astype(jnp.bfloat16)
        update = lax.all_gather(my_update, ("rows", "cols"), axis=0, tiled=True)
        chosen_norms = jnp.sum(jnp.square(chosen.astype(jnp.float32)), axis=1)

        def kernel_rows(operands):
            block_rows, block_norms = operands
            inner = lax.dot_general(
                block_rows, chosen, (((1,), (1,)), ((), ())), preferred_element_type=jnp.float32
            )
            distance = block_norms[:, None] + chosen_norms[None, :] - 2.0 * inner
            kernel = jnp.exp(distance * exponent).astype(jnp.bfloat16)
            return jnp.dot(kernel, update, preferred_element_type=jnp.float32)

        change = lax.map(kernel_rows, (feature_blocks, norm_blocks)).reshape(frame_count, -1)
        residual = residual - change
        is_owner = jnp.where(my_row == owner_row, 1.0, 0.0).astype(jnp.float32)
        mine_update = (
            lax.dynamic_slice_in_dim(update, my_col * per_col, per_col, 0).astype(jnp.float32)
            * is_owner
        )
        residual = residual.at[chosen_rows].add(-penalty * mine_update)
        coeffs = coeffs.at[chosen_rows].add(mine_update)
    return (coeffs, residual)


def power_of_two(value):
    return value & (value - 1) == 0


def solution(mesh):
    rows, cols = mesh.shape["rows"], mesh.shape["cols"]
    in_specs = (
        P(("rows", "cols"), None),
        P(("rows", "cols"), None),
        P(("rows", "cols"), None),
        P(None, ("rows", "cols"), None),
        P(None, "cols"),
        P(),
    )
    out_specs = (P(("rows", "cols"), None), P(("rows", "cols"), None))

    def per_device(features, residual, coeffs, block_inverse, block_index, owners):
        args = (features, residual, coeffs, block_inverse, block_index, owners)
        return per_device_pieces(rows, cols, *args) if fits(*args) else per_device_plain(*args)

    def fits(features, residual, coeffs, block_inverse, block_index, owners):
        return (
            small
            and block_index.shape[0] == 2
            and block_index.shape[1] % LANES == 0
            and 2 * block_inverse.shape[1] == LANES
            and features.shape[0] % 1024 == 0
        )

    small = power_of_two(rows) and power_of_two(cols) and 2 <= rows <= 8 and 4 <= cols <= 16
    return jax.shard_map(
        per_device, mesh=mesh, in_specs=in_specs, out_specs=out_specs, check_vma=False
    )
```

```python
import math

import jax
import jax.numpy as jnp
from jax import lax
from jax.experimental import pallas as pl
from jax.experimental.pallas import tpu as pltpu
from jax.sharding import PartitionSpec as P


penalty = 0.5
LANES = 128
VMEM = pltpu.MemorySpace.VMEM
SMEM = pltpu.MemorySpace.SMEM
f32 = jnp.float32
bf16 = jnp.bfloat16
f16 = jnp.float16
MM = dict(preferred_element_type=f32)


def up(value, unit):
    return -(-value // unit) * unit


def params(megabytes=20):
    return pltpu.CompilerParams(vmem_limit_bytes=megabytes * 1024 * 1024)


def split(value, parts):
    pieces = []
    for _ in range(parts - 1):
        high = value.astype(bf16)
        pieces.append(high)
        value = value - high.astype(f32)
    pieces.append(value.astype(bf16))
    return pieces


def matmul(a, b):
    return lax.dot_general(a, b, (((1,), (0,)), ((), ())), **MM)


def matmul_nt(a, b):
    return lax.dot_general(a, b, (((1,), (1,)), ((), ())), **MM)


def one_hot(frames, index_row):
    rows = lax.broadcasted_iota(jnp.int32, (frames, index_row.shape[1]), 0)
    return jnp.where(rows == index_row, 1.0, 0.0).astype(bf16)


def turn(row):
    square = jnp.broadcast_to(row.astype(f32), (LANES, row.shape[1]))
    return jnp.transpose(square)[:, 0:1].astype(jnp.int32)


def padded(value, rows):
    return jnp.pad(value, ((0, rows - value.shape[0]), (0, 0)))


vmem = pl.BlockSpec(memory_space=VMEM)
smem = pl.BlockSpec(memory_space=SMEM)


def pick_residual(index, residual_t):
    outputs, frames = residual_t.shape
    rows = up(outputs, 16)
    steps, picks = index.shape

    def body(index_hbm, residual_hbm, *refs):
        out_ref, (index_ref, residual_ref, index_sem, residual_sem) = refs[:steps], refs[steps:]
        index_copy = pltpu.make_async_copy(index_hbm, index_ref, index_sem)
        residual_copy = pltpu.make_async_copy(residual_hbm, residual_ref, residual_sem)
        residual_copy.start()
        index_copy.start()
        index_copy.wait()
        residual_copy.wait()
        both = jnp.concatenate(split(padded(residual_ref[...], rows), 2), 0)
        for step in range(steps):
            found = matmul(both, one_hot(frames, index_ref[step : step + 1, :]))
            out_ref[step][...] = found[:rows] + found[rows:]

    return pl.pallas_call(
        body,
        in_specs=[pl.BlockSpec(memory_space=pl.ANY)] * 2,
        out_specs=(vmem,) * steps,
        out_shape=(jax.ShapeDtypeStruct((rows, picks), f32),) * steps,
        scratch_shapes=[
            pltpu.VMEM((steps, picks), jnp.int32),
            pltpu.VMEM((outputs, frames), f32),
            pltpu.SemaphoreType.DMA,
            pltpu.SemaphoreType.DMA,
        ],
        compiler_params=params(),
        name="pick_residual",
    )(index, residual_t)


def norm_rows(squares, kinds):
    width = squares.shape[1]
    norm = split(-0.5 * squares, 3)
    ones = jnp.ones((3, width), bf16)
    zeros = jnp.zeros((6, width), bf16)
    norm = jnp.concatenate(norm, 0)
    pieces = []
    for kind in kinds:
        if kind == 0:
            pieces.append(zeros)
        elif kind == 1:
            pieces.append(jnp.concatenate([norm, ones], 0))
        else:
            pieces.append(jnp.concatenate([ones, norm], 0))
    return jnp.concatenate(pieces, 0)


def pick_features(owners, index, features_t, rules):
    width, frames = features_t.shape
    depth = up(width + 18, 16)
    steps, picks = index.shape
    kinds = ((2, 0, 1), (0, 2, 2))

    def body(owners_ref, index_ref, features_ref, *out_ref):
        features = features_ref[...]
        rest = jnp.zeros((depth - width - 18, picks), bf16)
        for step in range(steps):
            picked = matmul(features, one_hot(frames, index_ref[step : step + 1, :]))
            squares = jnp.sum(picked * picked, axis=0, keepdims=True)
            out_ref[step][0:width, :] = picked.astype(bf16)
            out_ref[step][width:depth, :] = jnp.concatenate([norm_rows(squares, kinds[step]), rest], 0)
        row = lax.axis_index("rows")
        for (step, rule), take_ref in zip(rules, out_ref[steps:]):
            take = jnp.where(rule(row, owners_ref[step]), 1.0, 0.0)
            take_ref[...] = jnp.full(take_ref.shape, take, f32)

    return pl.pallas_call(
        body,
        in_specs=[smem, vmem, vmem],
        out_specs=(vmem,) * (steps + len(rules)),
        out_shape=(jax.ShapeDtypeStruct((depth, picks), bf16),) * steps
        + (jax.ShapeDtypeStruct((1, picks), f32),) * len(rules),
        compiler_params=params(),
        name="pick_features",
    )(owners, index, features_t)


def lane_start(value, unit):
    return pl.ds(pl.multiple_of(value * unit, unit), unit)


def piece_col(piece):
    mine = lax.axis_index("cols")
    return ((mine // 2) ^ (piece // 2)) * 2 + ((mine % 2) ^ (piece % 2))


def fold(update):
    half = update.shape[0] // 2
    return jnp.concatenate([update[:half], update[half:]], 1).astype(bf16)


def localize(features_t):
    width, frames = features_t.shape
    depth = up(width + 18, 16)

    def body(features_ref, local_ref):
        features = features_ref[...]
        wide = features.astype(f32)
        squares = jnp.sum(wide * wide, axis=0, keepdims=True)
        local_ref[0:width, :] = features
        rest = jnp.zeros((depth - width - 18, frames), bf16)
        local_ref[width:depth, :] = jnp.concatenate([norm_rows(squares, (1, 1, 0)), rest], 0)

    return pl.pallas_call(
        body,
        in_specs=[vmem],
        out_specs=vmem,
        out_shape=jax.ShapeDtypeStruct((depth, frames), bf16),
        compiler_params=params(),
        name="localize",
    )(features_t)


def prepare(inverse, picks):
    steps, mine, block = inverse.shape

    def body(inverse_ref, *stacked_ref):
        for step in range(steps):
            for k in range(block // picks):
                high, low = split(inverse_ref[step, :, lane_start(piece_col(k), picks)], 2)
                stacked_ref[step][:, k * picks : (k + 1) * picks] = jnp.concatenate([high, low], 0)

    return pl.pallas_call(
        body,
        in_specs=[vmem],
        out_specs=(vmem,) * steps,
        out_shape=(jax.ShapeDtypeStruct((2 * mine, block), bf16),) * steps,
        compiler_params=params(),
        name="prepare",
    )(inverse)


def block_update(picked, stacked, scaled):
    rows, _ = picked.shape
    mine = stacked.shape[0] // 2

    def body(stacked_ref, picked_ref, out_ref):
        product = matmul_nt(jnp.concatenate(split(picked_ref[...], 2), 0), stacked_ref[...])
        product = product[:rows] + product[rows:]
        out_ref[...] = fold((product[:, :mine] + product[:, mine:]) * scaled)

    return pl.pallas_call(
        body,
        in_specs=[vmem, vmem],
        out_specs=vmem,
        out_shape=jax.ShapeDtypeStruct((rows // 2, 2 * mine), bf16),
        compiler_params=params(),
    )(stacked, picked)


def meeting_kernel(owners, index, pieces, second, scale):
    depth, picks = second.shape
    count = len(pieces)

    def body(owners_ref, index_ref, second_ref, *refs):
        pieces_ref, out_ref = refs[:count], refs[-1]
        for k in range(count):
            inner = matmul(jnp.transpose(pieces_ref[k][...]), second_ref[...])
            kernel = jnp.exp2(inner * scale).astype(bf16)
            if k == 0:
                same = turn(index_ref[0:1, :]) == index_ref[1:2, :]
                bonus = jnp.where(owners_ref[0] == owners_ref[1], penalty, 0.0)
                kernel = kernel + jnp.where(same, bonus, 0.0).astype(bf16)
            out_ref[k * picks : (k + 1) * picks, :] = kernel

    return pl.pallas_call(
        body,
        in_specs=[smem, vmem, vmem] + [vmem] * count,
        out_specs=vmem,
        out_shape=jax.ShapeDtypeStruct((count * picks, picks), bf16),
        cost_estimate=pl.CostEstimate(
            flops=2 * count * picks * picks * depth, transcendentals=count * picks * picks, bytes_accessed=10**6
        ),
        compiler_params=params(),
        name="meeting_kernel",
    )(owners, index, second, *pieces)


def advance(kernel, before, pieces, scaled):
    rows, picks = before.shape
    block = kernel.shape[0]
    count = len(pieces)

    def body(kernel_ref, before_ref, *refs):
        pieces_ref, out_ref, canon = refs[:count], refs[-2], refs[-1]
        unfold(pieces_ref, pieces[0].shape[0] * 2 // rows, picks, canon)
        out_ref[...] = (before_ref[...] - matmul(canon[...], kernel_ref[...])) * scaled

    return pl.pallas_call(
        body,
        in_specs=[vmem] * (2 + count),
        out_specs=vmem,
        out_shape=jax.ShapeDtypeStruct((rows, picks), f32),
        scratch_shapes=[pltpu.VMEM((rows, block), bf16)],
        compiler_params=params(),
        name="advance",
    )(kernel, before, *pieces)


def block_kernel(pieces, local, scale):
    depth, frames = local.shape
    picks = pieces[0].shape[1]
    count = len(pieces)
    block = picks * count
    tile = min(512, frames)

    def body(local_ref, *refs):
        pieces_ref, out_ref = refs[:count], refs[-1]
        for k in range(count):
            turned = jnp.transpose(pieces_ref[k][...])
            for start in range(0, frames, tile):
                inner = matmul(turned, local_ref[:, start : start + tile])
                out_ref[k * picks : (k + 1) * picks, start : start + tile] = jnp.exp2(inner * scale).astype(bf16)

    return pl.pallas_call(
        body,
        in_specs=[vmem] * (1 + count),
        out_specs=vmem,
        out_shape=jax.ShapeDtypeStruct((block, frames), bf16),
        cost_estimate=pl.CostEstimate(
            flops=2 * block * frames * depth, transcendentals=block * frames, bytes_accessed=10**7
        ),
        compiler_params=params(),
    )(local, *pieces)


def unfold(pieces_ref, parts, picks, canon):
    half, width = pieces_ref[0].shape[0] // parts, pieces_ref[0].shape[1]
    mine = width // 2
    count = len(pieces_ref)
    lanes = lax.broadcasted_iota(jnp.int32, (half, width), 1)
    low = lanes < mine
    row, col = lax.axis_index("rows"), lax.axis_index("cols")
    core = col % 2
    for k in range(0, count, 2):
        for r in range(parts):
            here = pieces_ref[k][r * half : (r + 1) * half, :].astype(f32)
            other = pieces_ref[k + 1][r * half : (r + 1) * half, :].astype(f32)
            a = jnp.where(core == 0, here, other)
            b = jnp.where(core == 0, other, here)
            upper = jnp.where(low, a, pltpu.roll(b, mine, 1))
            lower = jnp.where(low, pltpu.roll(a, mine, 1), b)
            pair = (row ^ r) * (count // 2) + ((col // 2) ^ (k // 2))
            from_col = pair * width // picks
            place = ((from_col // 2) ^ (col // 2)) * 2 + ((from_col % 2) ^ core)
            place = pl.ds(pl.multiple_of(place * picks + pair * width % picks, width), width)
            canon[0:half, place] = upper.astype(bf16)
            canon[half:, place] = lower.astype(bf16)


def apply_update(owners, pieces, kernels, index, step, residual_t, coeffs_t):
    outputs, frames = residual_t.shape
    block = sum(kernel.shape[0] for kernel in kernels)
    picks = index.shape[1]
    count = len(pieces)
    rows = up(outputs, 16)
    tile = min(512, frames)
    tiles = frames // tile

    def body(owners_ref, index_ref, residual_ref, coeffs_ref, *refs):
        kernels_ref, refs = refs[: len(kernels)], refs[len(kernels) :]
        pieces_ref = refs[:count]
        out_residual, out_coeffs, canon, new_residual, new_coeffs, sems = refs[count:]
        unfold(pieces_ref, pieces[0].shape[0] * 2 // rows, picks, canon)
        mine = canon[:, 0:picks]
        own = jnp.where(lax.axis_index("rows") == owners_ref[step], mine, jnp.zeros_like(mine))
        places = turn(index_ref[step : step + 1, :])
        copies = []
        for n in range(tiles):
            here = slice(n * tile, (n + 1) * tile)
            change, first = 0.0, 0
            for kernel_ref in kernels_ref:
                last = first + kernel_ref.shape[0]
                change = change + matmul(canon[:, first:last], kernel_ref[:, here])
                first = last
            frame = lax.broadcasted_iota(jnp.int32, (picks, tile), 1) + n * tile
            put = matmul(own, jnp.where(frame == places, 1.0, 0.0).astype(bf16))
            new_residual[:, here] = residual_ref[:, here] - (change + penalty * put)[:outputs]
            new_coeffs[:, here] = coeffs_ref[:, here] + put[:outputs]
            for k, (new, out) in enumerate(((new_residual, out_residual), (new_coeffs, out_coeffs))):
                copy = pltpu.make_async_copy(new.at[:, here], out.at[:, here], sems.at[2 * n + k])
                copy.start()
                copies.append(copy)
        for copy in copies:
            copy.wait()

    return pl.pallas_call(
        body,
        in_specs=[smem, vmem, vmem, vmem] + [vmem] * (len(kernels) + count),
        out_specs=(pl.BlockSpec(memory_space=pl.ANY),) * 2,
        out_shape=(jax.ShapeDtypeStruct((outputs, frames), f32),) * 2,
        scratch_shapes=[
            pltpu.VMEM((rows, block), bf16),
            pltpu.VMEM((outputs, frames), f32),
            pltpu.VMEM((outputs, frames), f32),
            pltpu.SemaphoreType.DMA((2 * tiles,)),
        ],
        cost_estimate=pl.CostEstimate(
            flops=2 * rows * block * frames, transcendentals=0, bytes_accessed=2 * block * frames
        ),
        compiler_params=params(),
    )(owners, index, residual_t, coeffs_t, *kernels, *pieces)


class Sender:
    def __init__(self, rows, cols):
        self.rows, self.cols, self.chips = rows, cols, cols // 2

    def send(self, value, row=None, chip_step=0, core_step=0):
        pairs = []
        for i in range(self.rows * self.cols):
            at, col = i // self.cols, i % self.cols
            to = at if row is None else row(at)
            if to is None:
                continue
            col = ((col // 2) ^ chip_step) * 2 + ((col % 2) ^ core_step)
            pairs.append((i, to * self.cols + col))
        return lax.ppermute(value, ("rows", "cols"), pairs)

    def spread(self, value, moves, takes):
        for move, take in zip(moves, takes):
            other = self.send(value, row=move)
            value = jnp.where(take > 0.5, other, value)
        return value

    def over_rows(self, value):
        steps = range(1, self.rows)
        got = {k: self.send(value, row=lambda at, k=k: at ^ k) for k in steps}
        return [value] + [got[k] for k in range(1, self.rows)]

    def over_cores(self, values):
        return [side for v in values for side in (v, self.send(v, core_step=1))]

    def over_cols(self, value):
        values = [value] + [self.send(value, chip_step=k) for k in range(1, self.chips)]
        return self.over_cores(values)


def doubling(rows):
    steps = [1 << k for k in range(rows.bit_length() - 1)]
    moves = [lambda at, step=step: at ^ step for step in steps]
    rules = [lambda row, owner, step=step: ((row ^ owner) & step) != 0 for step in steps]
    return moves, rules


def per_device_pieces(rows, cols, features, residual, coeffs, block_inverse, block_index, owners):
    scale = 2.0 / features.shape[1] * 1.4426950408889634
    sender = Sender(rows, cols)
    picks = block_index.shape[1]
    moves, rules = doubling(rows)
    block = block_inverse.shape[2]
    bound = 6.0 + (block + penalty) * block * 6.0 * 0.0234375
    scaled = 2.0 ** -max(0, math.ceil(math.log2(bound / 60000.0)))
    features_t, residual_t, coeffs_t = features.T, residual.T, coeffs.T
    first, second = pick_residual(block_index, residual_t)
    first_block, second_block, *takes = pick_features(
        owners, block_index, features_t, [(step, rule) for step in range(2) for rule in rules]
    )
    stacked = prepare(block_inverse, picks)
    local = localize(features_t)
    first = sender.over_cols(sender.spread(first.astype(f16), moves, takes))
    first_block = sender.over_cols(sender.spread(first_block, moves, takes))
    depth = second_block.shape[0]
    both = jnp.concatenate([second_block.astype(f16), second.astype(f16)], 0)
    both = sender.spread(both, moves, takes[len(rules) :])
    second_block, second = both[:depth].astype(bf16), both[depth:].astype(f32)
    update = block_update(jnp.concatenate(first, 1).astype(f32), stacked[0], 1.0)
    update = sender.over_cols(jnp.concatenate(sender.over_rows(update), 0))
    meeting = meeting_kernel(owners, block_index, first_block, second_block, scale)
    second = sender.over_cols(advance(meeting, second, update, scaled).astype(f16))
    near = len(first_block) // 2
    near_kernel = block_kernel(first_block[:near], local, scale)
    far_kernel = block_kernel(first_block[near:], local, scale)
    later = block_update(jnp.concatenate(second, 1).astype(f32), stacked[1], 1.0 / scaled)
    later = sender.over_cols(jnp.concatenate(sender.over_rows(later), 0))
    second_block = sender.over_cols(second_block)
    second_kernel = block_kernel(second_block, local, scale)
    residual_t, coeffs_t = apply_update(
        owners, update, (near_kernel, far_kernel), block_index, 0, residual_t, coeffs_t
    )
    residual_t, coeffs_t = apply_update(
        owners, later, (second_kernel,), block_index, 1, residual_t, coeffs_t
    )
    return (coeffs_t.T, residual_t.T)


def from_root(value, axis, source):
    kept = jnp.where(lax.axis_index(axis) == source, value, 0).astype(value.dtype)
    return lax.psum(kept, axis)


def per_device_plain(features, residual, coeffs, block_inverse, block_index, owners):
    frame_count = features.shape[0]
    feature_width = features.shape[1]
    per_col = block_index.shape[1]
    row_block = min(512, frame_count)
    exponent = -1.0 / feature_width
    my_row = lax.axis_index("rows")
    my_col = lax.axis_index("cols")
    squares = jnp.sum(jnp.square(features.astype(jnp.float32)), axis=1)
    feature_blocks = features.reshape(frame_count // row_block, row_block, feature_width)
    norm_blocks = squares.reshape(frame_count // row_block, row_block)
    for step_id in range(block_index.shape[0]):
        chosen_rows = block_index[step_id]
        owner_row = owners[step_id]
        mine_feat = jnp.take(features, chosen_rows, axis=0)
        mine_res = jnp.take(residual, chosen_rows, axis=0)
        row_piece = from_root(mine_feat, "rows", owner_row)
        chosen = lax.all_gather(row_piece, "cols", axis=0, tiled=True)
        res_piece = from_root(mine_res, "rows", owner_row)
        picked_res = lax.all_gather(res_piece, "cols", axis=0, tiled=True)
        my_update = jnp.dot(
            block_inverse[step_id],
            picked_res,
            precision=lax.Precision.HIGHEST,
            preferred_element_type=jnp.float32,
        ).astype(jnp.bfloat16)
        update = lax.all_gather(my_update, ("rows", "cols"), axis=0, tiled=True)
        chosen_norms = jnp.sum(jnp.square(chosen.astype(jnp.float32)), axis=1)

        def kernel_rows(operands):
            block_rows, block_norms = operands
            inner = lax.dot_general(
                block_rows, chosen, (((1,), (1,)), ((), ())), preferred_element_type=jnp.float32
            )
            distance = block_norms[:, None] + chosen_norms[None, :] - 2.0 * inner
            kernel = jnp.exp(distance * exponent).astype(jnp.bfloat16)
            return jnp.dot(kernel, update, preferred_element_type=jnp.float32)

        change = lax.map(kernel_rows, (feature_blocks, norm_blocks)).reshape(frame_count, -1)
        residual = residual - change
        is_owner = jnp.where(my_row == owner_row, 1.0, 0.0).astype(jnp.float32)
        mine_update = (
            lax.dynamic_slice_in_dim(update, my_col * per_col, per_col, 0).astype(jnp.float32)
            * is_owner
        )
        residual = residual.at[chosen_rows].add(-penalty * mine_update)
        coeffs = coeffs.at[chosen_rows].add(mine_update)
    return (coeffs, residual)


def power_of_two(value):
    return value & (value - 1) == 0


def solution(mesh):
    rows, cols = mesh.shape["rows"], mesh.shape["cols"]
    in_specs = (
        P(("rows", "cols"), None),
        P(("rows", "cols"), None),
        P(("rows", "cols"), None),
        P(None, ("rows", "cols"), None),
        P(None, "cols"),
        P(),
    )
    out_specs = (P(("rows", "cols"), None), P(("rows", "cols"), None))

    def per_device(features, residual, coeffs, block_inverse, block_index, owners):
        args = (features, residual, coeffs, block_inverse, block_index, owners)
        return per_device_pieces(rows, cols, *args) if fits(*args) else per_device_plain(*args)

    def fits(features, residual, coeffs, block_inverse, block_index, owners):
        return (
            small
            and block_index.shape[0] == 2
            and block_index.shape[1] % LANES == 0
            and 2 * block_inverse.shape[1] == LANES
            and features.shape[0] % 512 == 0
        )

    small = power_of_two(rows) and power_of_two(cols) and 2 <= rows <= 8 and 4 <= cols <= 16
    return jax.shard_map(
        per_device, mesh=mesh, in_specs=in_specs, out_specs=out_specs, check_vma=False
    )
```
